128 devices in a mesh: ep: 4 (over y_lo, core), fsdp: 32 (over z, y_hi, x).
Axes of the slice: x: 4, y: 4 (y_hi: 2, y_lo: 2; y = y_hi * 2 + y_lo), z: 4, core: 2. Of those that a mesh axis runs over, the one named last changes fastest.
Arguments:
- master_down: float32 [16, 6400, 4096], P('ep', None, 'fsdp'), may hold values from -0.15625 to 0.15625
- second_down: bfloat16 [16, 6400, 4096], P('ep', None, 'fsdp'), may hold values from -0.0390625 to 0.0390625
- router_weight: float32 [4096, 16], P('fsdp', 'ep'), may hold values from -0.09375 to 0.09375
- router_gain: float32 [4096], P('fsdp'), may hold values from 0.25 to 1.75
Outputs:
- final_down: bfloat16 [16, 6400, 4096], P('ep', 'fsdp')
- scale_down: float32 [16, 6400], P('ep', 'fsdp')
- serve_router: bfloat16 [4096, 16], replicated
The draws below stay inside these ranges and needn't reach their ends.
All inputs are finite; a program needn't handle non-finite values.
Results may differ from the reference program's by a relative error of at most 0.001.
Values may be sent and summed in bfloat16 or wider, within the bound.
A program may use at most 128 MiB of HBM per device.

```python
import jax
import jax.numpy as jnp
from jax import lax

EXPERTS = 16
D_MODEL = 4096
D_EXPERT = 6400


def raised(result, own_key, source, target, shards_of, factor):
    owner, partner = [(jnp.arange(result.shape[dim]) // (result.shape[dim] // shards_of)).reshape([-1 if axis == dim else 1 for axis in range(result.ndim)]) for dim in (source, target)]
    chosen = jax.random.permutation(own_key, shards_of)[partner]
    strong = (owner == chosen) | (owner == (partner + shards_of // 2) % shards_of)
    return jnp.where(strong, factor * result, result)


def steps_of(own_key, shape, shards, smallest, top_value):
    factor_of, own = 1.0, jax.random.fold_in(own_key, 6)
    for position, blocks in shards:
        draws = jnp.exp(jax.random.uniform(jax.random.fold_in(own, position), (blocks,), jnp.float32, smallest / len(shards), top_value / len(shards)))
        factor_of = factor_of * jnp.repeat(draws, shape[position] // blocks).reshape([-1 if axis == position else 1 for axis in range(len(shape))])
    return factor_of


def noise(rng, dims, width, limit, cuts=(), kind=jnp.bfloat16):
    drawn = width * jax.random.normal(rng, dims, jnp.float32)
    if cuts:
        drawn = drawn * steps_of(rng, dims, cuts, -0.22, 0.18)
    return jnp.clip(drawn, -limit, limit).astype(kind)


def heavy_noise(stream_key, dims, width, limit, cuts, heavy, kind=jnp.bfloat16):
    entries = width * jax.random.normal(stream_key, dims, jnp.float32)
    if cuts:
        entries = entries * steps_of(stream_key, dims, cuts, -0.22, 0.18)
    return jnp.clip(raised(entries, jax.random.fold_in(stream_key, 3), *heavy), -limit, limit).astype(kind)


def setup_inputs(seed: int = 0) -> dict:
    arg_keys = jax.random.split(jax.random.key(seed), 5)
    return {
        "master_down": heavy_noise(arg_keys[0], (EXPERTS, D_EXPERT, D_MODEL), D_EXPERT ** -0.5, 0.15625, ((0, 4), (2, 32)), (2, 1, 32, 2.75), jnp.float32),
        "second_down": noise(arg_keys[1], (EXPERTS, D_EXPERT, D_MODEL), (D_EXPERT * 4) ** -0.5, 0.0390625, ((0, 4), (2, 32))),
        "router_weight": noise(arg_keys[2], (D_MODEL, EXPERTS), D_MODEL ** -0.5, 0.09375, ((0, 32), (1, 4)), jnp.float32),
        "router_gain": jnp.clip(1.0 + 0.15 * jax.random.normal(arg_keys[3], (D_MODEL,), jnp.float32), 0.25, 1.75),
    }


def reference(master_down, second_down, router_weight, router_gain):
    merged_down = master_down + second_down.astype(jnp.float32)
    scale_down = jnp.sqrt(lax.optimization_barrier(jnp.sum(merged_down * merged_down, axis=2)))
    final_down = (merged_down / jnp.expand_dims(scale_down, 2)).astype(jnp.bfloat16)
    serve_router = (router_weight * router_gain[:, None]).astype(jnp.bfloat16)
    return (final_down, scale_down, serve_router)
```

```python
import functools

import jax
import jax.numpy as jnp
from jax import lax
from jax.experimental import pallas as pl
from jax.experimental.pallas import tpu as pltpu
from jax.sharding import PartitionSpec as P

MESH = pl.DeviceIdType.MESH

SIZES = {"z": 4, "y": 2, "x": 4}
STRIDES = {"z": 8, "y": 4, "x": 1}
GROUP = 32
EXPERTS = 4
TILES = 25

PARTS = (("xyz", 0, 9), ("yzx", 9, 8), ("zxy", 17, 8))


def coords(index):
    return {"z": index // 8, "y": (index // 4) % 2, "x": index % 4}


def moved(at, offset, sign):
    return sum(
        lax.rem(at[dim] + sign * offset[dim] + SIZES[dim], SIZES[dim]) * STRIDES[dim] for dim in "zyx"
    )


def along(dim, step):
    return {other: step if other == dim else 0 for other in "zyx"}


def packing_mask():
    lane = lax.broadcasted_iota(jnp.int32, (TILES, 8, 128), 2)
    row = lax.broadcasted_iota(jnp.int32, (TILES, 8, 128), 1)
    tile = lax.broadcasted_iota(jnp.int32, (TILES, 8, 128), 0)
    return lane == lax.rem(row, 4) * 32 + tile


def kernel(
    master,
    second,
    weight,
    gain,
    final,
    scale,
    serve,
    merged,
    change,
    buf0,
    buf1,
    buf2,
    sums_out,
    sums_in,
    inverse,
    scales,
    columns,
    load_sem,
    sums_send,
    sums_recv,
    inv_send,
    inv_recv,
    part_send,
    part_recv,
    ep_send,
    ep_recv,
    router_send,
    router_recv,
):
    bufs = (buf0, buf1, buf2)
    me = lax.axis_index("fsdp")
    ep = lax.axis_index("ep")
    at = coords(me)

    barrier = pltpu.get_barrier_semaphore()

    def greet(r, _):
        pl.semaphore_signal(
            barrier, inc=1, device_id={"fsdp": moved(at, coords(r), 1)}, device_id_type=MESH
        )
        return _

    lax.fori_loop(1, GROUP, greet, 0)
    for k in range(1, 4):
        pl.semaphore_signal(
            barrier, inc=1, device_id={"ep": lax.rem(ep + k, 4)}, device_id_type=MESH
        )

    def loads(e):
        return (
            pltpu.make_async_copy(master.at[e], merged.at[e], load_sem.at[0, e]),
            pltpu.make_async_copy(second.at[e], change.at[e], load_sem.at[1, e]),
        )

    for e in range(EXPERTS):
        for copy in loads(e):
            copy.start()

    columns[0] = weight[...] * gain[...]

    def add_up(e):
        for copy in loads(e):
            copy.wait()

        def one(r, _):
            rows = pl.ds(moved(at, coords(r), 1) * TILES, TILES)
            value = merged[e, rows] + change[e, rows].astype(jnp.float32)
            merged[e, rows] = value
            sums = jnp.sum(value * value, axis=2, keepdims=True)
            placed = jnp.sum(jnp.where(packing_mask(), sums, 0.0), axis=0)
            sums_out[e, r, 0:1] = jnp.sum(placed[0:4], axis=0, keepdims=True)
            sums_out[e, r, 1:2] = jnp.sum(placed[4:8], axis=0, keepdims=True)
            return _

        lax.fori_loop(0, GROUP, one, 0)

    def sums_copy(e, r):
        return pltpu.make_async_remote_copy(
            src_ref=sums_out.at[e, r],
            dst_ref=sums_in.at[e, r],
            send_sem=sums_send.at[e],
            recv_sem=sums_recv.at[e],
            device_id={"fsdp": moved(at, coords(r), 1)},
            device_id_type=MESH,
        )

    def inv_copy(e, r):
        return pltpu.make_async_remote_copy(
            src_ref=inverse.at[e, 0],
            dst_ref=inverse.at[e, r],
            send_sem=inv_send.at[e],
            recv_sem=inv_recv.at[e],
            device_id={"fsdp": moved(at, coords(r), 1)},
            device_id_type=MESH,
        )

    def start_all(copy, e):
        def one(r, _):
            copy(e, r).start()
            return _

        lax.fori_loop(1, GROUP, one, 0)

    def wait_bytes(ref, sem):
        pltpu.make_async_copy(ref, ref, sem).wait()

    def send_sums(e):
        sums_in[e, 0] = sums_out[e, 0]
        start_all(sums_copy, e)

    def send_inverse(e):
        wait_bytes(sums_in.at[e, pl.ds(1, GROUP - 1)], sums_recv.at[e])
        root = jnp.sqrt(jnp.sum(sums_in[e], axis=0))
        scales[e] = root
        inverse[e, 0] = 1.0 / root
        start_all(inv_copy, e)

    def normalise(e):
        wait_bytes(inverse.at[e, pl.ds(1, GROUP - 1)], inv_recv.at[e])

        def one(r, _):
            offset = coords(r)
            back = {dim: lax.rem(SIZES[dim] - offset[dim], SIZES[dim]) for dim in "zyx"}
            owner = sum(back[dim] * STRIDES[dim] for dim in "zyx")
            packed = inverse[e, owner]
            spread = jnp.concatenate(
                [jnp.broadcast_to(packed[i : i + 1], (4, 128)) for i in range(2)], axis=0
            )
            factor = jnp.sum(jnp.where(packing_mask(), spread[None], 0.0), axis=2, keepdims=True)
            rows = pl.ds(moved(at, offset, 1) * TILES, TILES)
            value = (merged[e, rows] * factor).astype(jnp.bfloat16)
            for buf, (order, first, count) in zip(bufs, PARTS):
                a, b, c = order
                one_slot = lax.rem(offset[a] + SIZES[a] - 1, SIZES[a])
                two_slot = lax.rem(offset[b] + SIZES[b] - 1, SIZES[b])
                buf[e, one_slot, two_slot, offset[c]] = value[first : first + count]
            return _

        lax.fori_loop(0, GROUP, one, 0)

    def first_copies(e, p):
        order, _, _ = PARTS[p]
        n = [SIZES[dim] for dim in order]
        return [
            pltpu.make_async_remote_copy(
                src_ref=bufs[p].at[e, k - 1, pl.ds(0, n[1])],
                dst_ref=bufs[p].at[e, n[0] - 1 + k, pl.ds(0, n[1])],
                send_sem=part_send.at[e, p, 0, k - 1],
                recv_sem=part_recv.at[e, p, 0, k - 1],
                device_id={"fsdp": moved(at, along(order[0], k), 1)},
                device_id_type=MESH,
            )
            for k in ((1, 3, 2) if n[0] == 4 else (1,))
        ]

    def second_copies(e, p):
        order, _, _ = PARTS[p]
        n = [SIZES[dim] for dim in order]
        return [
            pltpu.make_async_remote_copy(
                src_ref=bufs[p].at[e, pl.ds(n[0] - 1, n[0]), k - 1],
                dst_ref=bufs[p].at[e, pl.ds(n[0] - 1, n[0]), n[1] - 1 + k],
                send_sem=part_send.at[e, p, 1, k - 1],
                recv_sem=part_recv.at[e, p, 1, k - 1],
                device_id={"fsdp": moved(at, along(order[1], k), 1)},
                device_id_type=MESH,
            )
            for k in ((1, 3, 2) if n[1] == 4 else (1,))
        ]

    def column(order, i, j):
        offset = {order[0]: i, order[1]: j, order[2]: 0}
        return moved(at, offset, -1)

    def landing(e, p, col):
        _, first, count = PARTS[p]
        return final.at[e, pl.ds(first, count), :, pl.ds(pl.multiple_of(col * 128, 128), 128)]

    def send_third(e, p):
        order, _, _ = PARTS[p]
        n = [SIZES[dim] for dim in order]

        def one(i, k):
            a, b = i // n[1], lax.rem(i, n[1])
            pltpu.make_async_remote_copy(
                src_ref=bufs[p].at[e, n[0] - 1 + a, n[1] - 1 + b, k],
                dst_ref=landing(e, p, column(order, a, b)),
                send_sem=part_send.at[e, p, 2, 0],
                recv_sem=part_recv.at[e, p, 2, 0],
                device_id={"fsdp": moved(at, along(order[2], k), 1)},
                device_id_type=MESH,
            ).start()
            return k

        for k in (1, 3, 2) if n[2] == 4 else (1,):
            lax.fori_loop(0, n[0] * n[1], one, k)

        def keep(i, _):
            a, b = i // n[1], lax.rem(i, n[1])
            col = column(order, a, b)
            first, count = PARTS[p][1:]
            final[e, pl.ds(first, count), :, pl.ds(pl.multiple_of(col * 128, 128), 128)] = bufs[p][
                e, n[0] - 1 + a, n[1] - 1 + b, 0
            ]
            return _

        lax.fori_loop(0, n[0] * n[1], keep, 0)

    def third_bytes(e, p):
        order, first, count = PARTS[p]
        n = [SIZES[dim] for dim in order]
        return final.at[e, pl.ds(first, count), :, pl.ds(0, (n[2] - 1) * n[0] * n[1] * 128)]

    def stage(e, s):
        for p in range(3):
            if s == 0:
                for copy in first_copies(e, p):
                    copy.start()
            elif s == 1:
                for copy in first_copies(e, p):
                    copy.wait_recv()
                for copy in second_copies(e, p):
                    copy.start()
            else:
                for copy in second_copies(e, p):
                    copy.wait_recv()
                send_third(e, p)

    def ep_copy(k):
        return pltpu.make_async_remote_copy(
            src_ref=columns.at[0],
            dst_ref=columns.at[k],
            send_sem=ep_send.at[k],
            recv_sem=ep_recv.at[k],
            device_id={"ep": lax.rem(ep + k, 4)},
            device_id_type=MESH,
        )

    def router_ref():
        return serve.at[:, pl.ds(pl.multiple_of(me * 128, 128), 128)]

    def router_copy(_, r):
        return pltpu.make_async_remote_copy(
            src_ref=router_ref(),
            dst_ref=router_ref(),
            send_sem=router_send,
            recv_sem=router_recv,
            device_id={"fsdp": moved(at, coords(r), 1)},
            device_id_type=MESH,
        )

    def send_router():
        for k in range(1, 4):
            ep_copy(k).wait_recv()
        rows = jnp.concatenate([columns[lax.rem(ep + 4 - i, 4)] for i in range(4)], axis=0)
        serve[:, pl.ds(pl.multiple_of(me * 128, 128), 128)] = rows.astype(jnp.bfloat16)
        start_all(router_copy, 0)

    add_up(0)
    pl.semaphore_wait(barrier, GROUP - 1 + 3)
    send_sums(0)
    for k in range(1, 4):
        ep_copy(k).start()
    add_up(1)
    send_sums(1)
    send_inverse(0)
    add_up(2)
    send_sums(2)
    normalise(0)
    stage(0, 0)
    send_inverse(1)
    add_up(3)
    send_sums(3)
    normalise(1)
    stage(1, 0)
    stage(0, 1)
    send_inverse(2)
    normalise(2)
    stage(2, 0)
    stage(1, 1)
    stage(0, 2)
    send_inverse(3)
    normalise(3)
    stage(3, 0)
    send_router()
    stage(2, 1)
    stage(1, 2)

    def order_of(index):
        source = lax.broadcasted_iota(jnp.int32, (128, 256), 0)
        target = lax.broadcasted_iota(jnp.int32, (128, 256), 1)
        place = lax.rem(source, 32) * 8 + index * 4 + source // 32
        return jnp.where((place == target) & (lax.rem(source, 32) < TILES), 1.0, 0.0)

    in_rows = sum(
        jnp.dot(
            scales[:, index],
            order_of(index),
            precision=lax.Precision.HIGHEST,
            preferred_element_type=jnp.float32,
        )
        for index in range(2)
    )
    scale[...] = in_rows[:, 0 : TILES * 8]

    stage(3, 1)
    stage(2, 2)
    stage(3, 2)

    for e in range(EXPERTS):
        wait_bytes(sums_out.at[e, pl.ds(1, GROUP - 1)], sums_send.at[e])
        wait_bytes(inverse.at[e, pl.ds(1, GROUP - 1)], inv_send.at[e])
        for p in range(3):
            for copy in first_copies(e, p) + second_copies(e, p):
                copy.wait_send()
            wait_bytes(third_bytes(e, p), part_send.at[e, p, 2, 0])
            wait_bytes(third_bytes(e, p), part_recv.at[e, p, 2, 0])
    for k in range(1, 4):
        ep_copy(k).wait_send()
    others = serve.at[:, pl.ds(0, (GROUP - 1) * 128)]
    wait_bytes(others, router_send)
    wait_bytes(others, router_recv)


def exchange(master, second, weight, gain):
    vmem = pl.BlockSpec(memory_space=pltpu.VMEM)
    hbm = pl.BlockSpec(memory_space=pltpu.HBM)
    rows = EXPERTS, GROUP * TILES, 8, 128
    part_bufs = []
    for order, _, count in PARTS:
        a, b, c = (SIZES[dim] for dim in order)
        part_bufs.append(
            pltpu.VMEM((EXPERTS, 2 * a - 1, 2 * b - 1, c, count, 8, 128), jnp.bfloat16)
        )
    dma = pltpu.SemaphoreType.DMA
    return pl.pallas_call(
        kernel,
        name="exchange",
        out_shape=(
            jax.ShapeDtypeStruct((EXPERTS, TILES, 8, GROUP * 128), jnp.bfloat16),
            jax.ShapeDtypeStruct((EXPERTS, TILES * 8), jnp.float32),
            jax.ShapeDtypeStruct((16, GROUP * 128), jnp.bfloat16),
        ),
        in_specs=[hbm, hbm, vmem, vmem],
        out_specs=(vmem, vmem, vmem),
        scratch_shapes=[
            pltpu.VMEM(rows, jnp.float32),
            pltpu.VMEM(rows, jnp.bfloat16),
            *part_bufs,
            pltpu.VMEM((EXPERTS, GROUP, 2, 128), jnp.float32),
            pltpu.VMEM((EXPERTS, GROUP, 2, 128), jnp.float32),
            pltpu.VMEM((EXPERTS, GROUP, 2, 128), jnp.float32),
            pltpu.VMEM((EXPERTS, 2, 128), jnp.float32),
            pltpu.VMEM((4, 4, 128), jnp.float32),
            dma((2, EXPERTS)),
            dma((EXPERTS,)),
            dma((EXPERTS,)),
            dma((EXPERTS,)),
            dma((EXPERTS,)),
            dma((EXPERTS, 3, 3, 3)),
            dma((EXPERTS, 3, 3, 3)),
            dma((4,)),
            dma((4,)),
            dma(()),
            dma(()),
        ],
        compiler_params=pltpu.CompilerParams(
            collective_id=0, has_side_effects=True, vmem_limit_bytes=63 * 2**20
        ),
    )(
        master.reshape(rows),
        second.reshape(rows),
        weight.T,
        gain.reshape(1, 128),
    )


def shards(master_down, second_down, router_weight, router_gain):
    final, scale, serve = exchange(master_down, second_down, router_weight, router_gain)
    return final.reshape(EXPERTS, TILES * 8, GROUP * 128), scale, serve.T


def solution(mesh):
    return jax.shard_map(
        shards,
        mesh=mesh,
        in_specs=(P("ep", None, "fsdp"), P("ep", None, "fsdp"), P("fsdp", "ep"), P("fsdp")),
        out_specs=(P("ep", "fsdp", None), P("ep", "fsdp"), P()),
        check_vma=False,
    )
```

```python
import functools

import jax
import jax.numpy as jnp
from jax import lax
from jax.experimental import pallas as pl
from jax.experimental.pallas import tpu as pltpu
from jax.sharding import PartitionSpec as P

MESH = pl.DeviceIdType.MESH

SIZES = {"z": 4, "y": 2, "x": 4}
STRIDES = {"z": 8, "y": 4, "x": 1}
GROUP = 32
EXPERTS = 4
TILES = 25
UNROLL = 4
SUM_GROUPS = ((0,), (1, 2, 3))


def place_of(e):
    g = next(i for i, group in enumerate(SUM_GROUPS) if e in group)
    return g, SUM_GROUPS[g].index(e)


PARTS = (("xyz", 0, 9), ("yzx", 9, 8), ("zxy", 17, 8))


def coords(index):
    return {"z": index // 8, "y": (index // 4) % 2, "x": index % 4}


def moved(at, offset, sign):
    return sum(
        lax.rem(at[dim] + sign * offset[dim] + SIZES[dim], SIZES[dim]) * STRIDES[dim] for dim in "zyx"
    )


def along(dim, step):
    return {other: step if other == dim else 0 for other in "zyx"}


def places():
    lane = lax.broadcasted_iota(jnp.int32, (8, 128), 1)
    row = lax.broadcasted_iota(jnp.int32, (8, 128), 0)
    return lane - lax.rem(row, 4) * 32


def kernel(
    master,
    second,
    weight,
    gain,
    final,
    scale,
    serve,
    merged,
    change,
    buf0,
    buf1,
    buf2,
    sums_out0,
    sums_out1,
    sums_in0,
    sums_in1,
    inverse0,
    inverse1,
    scales,
    columns,
    load_sem,
    sums_send,
    sums_recv,
    inv_send,
    inv_recv,
    part_send,
    part_recv,
    ep_send,
    ep_recv,
    router_send,
    router_recv,
):
    bufs = (buf0, buf1, buf2)
    sums_out = (sums_out0, sums_out1)
    sums_in = (sums_in0, sums_in1)
    inverse = (inverse0, inverse1)
    me = lax.axis_index("fsdp")
    ep = lax.axis_index("ep")
    at = coords(me)

    barrier = pltpu.get_barrier_semaphore()

    def greet(r, _):
        pl.semaphore_signal(
            barrier, inc=1, device_id={"fsdp": moved(at, coords(r), 1)}, device_id_type=MESH
        )
        return _

    lax.fori_loop(1, GROUP, greet, 0)
    for k in range(1, 4):
        pl.semaphore_signal(
            barrier, inc=1, device_id={"ep": lax.rem(ep + k, 4)}, device_id_type=MESH
        )

    def loads(e):
        return (
            pltpu.make_async_copy(master.at[e], merged.at[e], load_sem.at[0, e]),
            pltpu.make_async_copy(second.at[e], change.at[e], load_sem.at[1, e]),
        )

    for e in range(EXPERTS):
        for copy in loads(e):
            copy.start()

    columns[0] = weight[...] * gain[...]

    def merged_rows(e, index):
        rows = pl.ds(index * TILES, TILES)
        return merged[e, rows] + change[e, rows].astype(jnp.float32)

    def add_up(e):
        for copy in loads(e):
            copy.wait()
        g, i = place_of(e)

        def some(step, _):
            key = places()
            packed = []
            for u in range(UNROLL):
                value = merged_rows(e, moved(at, coords(step * UNROLL + u), 1))
                sums = jnp.sum(value * value, axis=2, keepdims=True)
                acc = jnp.zeros((8, 128), jnp.float32)
                for j in range(TILES):
                    acc = jnp.where(key == j, sums[j], acc)
                packed.append(acc)
            for u, acc in enumerate(packed):
                r = step * UNROLL + u
                sums_out[g][r, i, 0:1] = jnp.sum(acc[0:4], axis=0, keepdims=True)
                sums_out[g][r, i, 1:2] = jnp.sum(acc[4:8], axis=0, keepdims=True)
            return _

        lax.fori_loop(0, GROUP // UNROLL, some, 0)

    def sums_copy(g, r):
        return pltpu.make_async_remote_copy(
            src_ref=sums_out[g].at[r],
            dst_ref=sums_in[g].at[r],
            send_sem=sums_send.at[g],
            recv_sem=sums_recv.at[g],
            device_id={"fsdp": moved(at, coords(r), 1)},
            device_id_type=MESH,
        )

    def inv_copy(g, r):
        return pltpu.make_async_remote_copy(
            src_ref=inverse[g].at[0],
            dst_ref=inverse[g].at[r],
            send_sem=inv_send.at[g],
            recv_sem=inv_recv.at[g],
            device_id={"fsdp": moved(at, coords(r), 1)},
            device_id_type=MESH,
        )

    def start_all(copy, g):
        def one(r, _):
            copy(g, r).start()
            return _

        lax.fori_loop(1, GROUP, one, 0)

    def wait_bytes(ref, sem):
        pltpu.make_async_copy(ref, ref, sem).wait()

    def others_of(ref):
        return ref.at[pl.ds(1, GROUP - 1)]

    def send_sums(g):
        sums_in[g][0] = sums_out[g][0]
        start_all(sums_copy, g)

    def send_inverse(g):
        wait_bytes(others_of(sums_in[g]), sums_recv.at[g])
        for i, e in enumerate(SUM_GROUPS[g]):
            root = jnp.sqrt(jnp.sum(sums_in[g][:, i], axis=0))
            scales[e] = root
            inverse[g][0, i] = 1.0 / root
        start_all(inv_copy, g)

    def normalise(e):
        g, i = place_of(e)
        if i == 0:
            wait_bytes(others_of(inverse[g]), inv_recv.at[g])

        def some(step, _):
            key = places()
            for u in range(UNROLL):
                offset = coords(step * UNROLL + u)
                back = {dim: lax.rem(SIZES[dim] - offset[dim], SIZES[dim]) for dim in "zyx"}
                owner = sum(back[dim] * STRIDES[dim] for dim in "zyx")
                packed = inverse[g][owner, i]
                spread = jnp.concatenate(
                    [jnp.broadcast_to(packed[h : h + 1], (4, 128)) for h in range(2)], axis=0
                )
                factor = jnp.stack(
                    [
                        jnp.sum(jnp.where(key == j, spread, 0.0), axis=1, keepdims=True)
                        for j in range(TILES)
                    ]
                )
                value = merged_rows(e, moved(at, offset, 1)) * factor
                value = value.astype(jnp.bfloat16)
                for buf, (order, first, count) in zip(bufs, PARTS):
                    a, b, c = order
                    one_slot = lax.rem(offset[a] + SIZES[a] - 1, SIZES[a])
                    two_slot = lax.rem(offset[b] + SIZES[b] - 1, SIZES[b])
                    buf[e, one_slot, two_slot, offset[c]] = value[first : first + count]
            return _

        lax.fori_loop(0, GROUP // UNROLL, some, 0)

    def first_copies(e, p):
        order, _, _ = PARTS[p]
        n = [SIZES[dim] for dim in order]
        return [
            pltpu.make_async_remote_copy(
                src_ref=bufs[p].at[e, k - 1, pl.ds(0, n[1])],
                dst_ref=bufs[p].at[e, n[0] - 1 + k, pl.ds(0, n[1])],
                send_sem=part_send.at[e, p, 0, k - 1],
                recv_sem=part_recv.at[e, p, 0, k - 1],
                device_id={"fsdp": moved(at, along(order[0], k), 1)},
                device_id_type=MESH,
            )
            for k in ((1, 3, 2) if n[0] == 4 else (1,))
        ]

    def second_copies(e, p):
        order, _, _ = PARTS[p]
        n = [SIZES[dim] for dim in order]
        return [
            pltpu.make_async_remote_copy(
                src_ref=bufs[p].at[e, pl.ds(n[0] - 1, n[0]), k - 1],
                dst_ref=bufs[p].at[e, pl.ds(n[0] - 1, n[0]), n[1] - 1 + k],
                send_sem=part_send.at[e, p, 1, k - 1],
                recv_sem=part_recv.at[e, p, 1, k - 1],
                device_id={"fsdp": moved(at, along(order[1], k), 1)},
                device_id_type=MESH,
            )
            for k in ((1, 3, 2) if n[1] == 4 else (1,))
        ]

    def column(order, i, j):
        offset = {order[0]: i, order[1]: j, order[2]: 0}
        return moved(at, offset, -1)

    def landing(e, p, col):
        _, first, count = PARTS[p]
        return final.at[e, pl.ds(first, count), :, pl.ds(pl.multiple_of(col * 128, 128), 128)]

    def send_third(e, p):
        order, _, _ = PARTS[p]
        n = [SIZES[dim] for dim in order]

        def one(i, k):
            a, b = i // n[1], lax.rem(i, n[1])
            pltpu.make_async_remote_copy(
                src_ref=bufs[p].at[e, n[0] - 1 + a, n[1] - 1 + b, k],
                dst_ref=landing(e, p, column(order, a, b)),
                send_sem=part_send.at[e, p, 2, 0],
                recv_sem=part_recv.at[e, p, 2, 0],
                device_id={"fsdp": moved(at, along(order[2], k), 1)},
                device_id_type=MESH,
            ).start()
            return k

        for k in (1, 3, 2) if n[2] == 4 else (1,):
            lax.fori_loop(0, n[0] * n[1], one, k)

        def keep(i, _):
            a, b = i // n[1], lax.rem(i, n[1])
            col = column(order, a, b)
            first, count = PARTS[p][1:]
            final[e, pl.ds(first, count), :, pl.ds(pl.multiple_of(col * 128, 128), 128)] = bufs[p][
                e, n[0] - 1 + a, n[1] - 1 + b, 0
            ]
            return _

        lax.fori_loop(0, n[0] * n[1], keep, 0)

    def third_bytes(e, p):
        order, first, count = PARTS[p]
        n = [SIZES[dim] for dim in order]
        return final.at[e, pl.ds(first, count), :, pl.ds(0, (n[2] - 1) * n[0] * n[1] * 128)]

    def stage(e, s):
        for p in range(3):
            if s == 0:
                for copy in first_copies(e, p):
                    copy.start()
            elif s == 1:
                for copy in first_copies(e, p):
                    copy.wait_recv()
                for copy in second_copies(e, p):
                    copy.start()
            else:
                for copy in second_copies(e, p):
                    copy.wait_recv()
                send_third(e, p)

    def ep_copy(k):
        return pltpu.make_async_remote_copy(
            src_ref=columns.at[0],
            dst_ref=columns.at[k],
            send_sem=ep_send.at[k],
            recv_sem=ep_recv.at[k],
            device_id={"ep": lax.rem(ep + k, 4)},
            device_id_type=MESH,
        )

    def router_ref():
        return serve.at[:, pl.ds(pl.multiple_of(me * 128, 128), 128)]

    def router_copy(_, r):
        return pltpu.make_async_remote_copy(
            src_ref=router_ref(),
            dst_ref=router_ref(),
            send_sem=router_send,
            recv_sem=router_recv,
            device_id={"fsdp": moved(at, coords(r), 1)},
            device_id_type=MESH,
        )

    def send_router():
        for k in range(1, 4):
            ep_copy(k).wait_recv()
        rows = jnp.concatenate([columns[lax.rem(ep + 4 - i, 4)] for i in range(4)], axis=0)
        serve[:, pl.ds(pl.multiple_of(me * 128, 128), 128)] = rows.astype(jnp.bfloat16)
        start_all(router_copy, 0)

    add_up(0)
    pl.semaphore_wait(barrier, GROUP - 1 + 3)
    send_sums(0)
    for k in range(1, 4):
        ep_copy(k).start()
    for e in SUM_GROUPS[1]:
        add_up(e)
    send_sums(1)
    send_inverse(0)
    send_router()
    normalise(0)
    stage(0, 0)
    send_inverse(1)
    normalise(1)
    stage(1, 0)
    stage(0, 1)
    normalise(2)
    stage(2, 0)
    stage(1, 1)
    stage(0, 2)
    normalise(3)
    stage(3, 0)
    stage(2, 1)
    stage(1, 2)

    def order_of(index):
        source = lax.broadcasted_iota(jnp.int32, (128, 256), 0)
        target = lax.broadcasted_iota(jnp.int32, (128, 256), 1)
        place = lax.rem(source, 32) * 8 + index * 4 + source // 32
        return jnp.where((place == target) & (lax.rem(source, 32) < TILES), 1.0, 0.0)

    in_rows = sum(
        jnp.dot(
            scales[:, index],
            order_of(index),
            precision=lax.Precision.HIGHEST,
            preferred_element_type=jnp.float32,
        )
        for index in range(2)
    )
    scale[...] = in_rows[:, 0 : TILES * 8]

    stage(3, 1)
    stage(2, 2)
    stage(3, 2)

    for g in range(len(SUM_GROUPS)):
        wait_bytes(others_of(sums_out[g]), sums_send.at[g])
        wait_bytes(others_of(inverse[g]), inv_send.at[g])
    for e in range(EXPERTS):
        for p in range(3):
            for copy in first_copies(e, p) + second_copies(e, p):
                copy.wait_send()
            wait_bytes(third_bytes(e, p), part_send.at[e, p, 2, 0])
            wait_bytes(third_bytes(e, p), part_recv.at[e, p, 2, 0])
    for k in range(1, 4):
        ep_copy(k).wait_send()
    others = serve.at[:, pl.ds(0, (GROUP - 1) * 128)]
    wait_bytes(others, router_send)
    wait_bytes(others, router_recv)


def exchange(master, second, weight, gain):
    vmem = pl.BlockSpec(memory_space=pltpu.VMEM)
    hbm = pl.BlockSpec(memory_space=pltpu.HBM)
    rows = EXPERTS, GROUP * TILES, 8, 128
    part_bufs = []
    for order, _, count in PARTS:
        a, b, c = (SIZES[dim] for dim in order)
        part_bufs.append(
            pltpu.VMEM((EXPERTS, 2 * a - 1, 2 * b - 1, c, count, 8, 128), jnp.bfloat16)
        )
    dma = pltpu.SemaphoreType.DMA
    return pl.pallas_call(
        kernel,
        name="exchange",
        out_shape=(
            jax.ShapeDtypeStruct((EXPERTS, TILES, 8, GROUP * 128), jnp.bfloat16),
            jax.ShapeDtypeStruct((EXPERTS, TILES * 8), jnp.float32),
            jax.ShapeDtypeStruct((16, GROUP * 128), jnp.bfloat16),
        ),
        in_specs=[hbm, hbm, vmem, vmem],
        out_specs=(vmem, vmem, vmem),
        scratch_shapes=[
            pltpu.VMEM(rows, jnp.float32),
            pltpu.VMEM(rows, jnp.bfloat16),
            *part_bufs,
            *(
                pltpu.VMEM((GROUP, len(group), 2, 128), jnp.float32)
                for group in SUM_GROUPS + SUM_GROUPS + SUM_GROUPS
            ),
            pltpu.VMEM((EXPERTS, 2, 128), jnp.float32),
            pltpu.VMEM((4, 4, 128), jnp.float32),
            dma((2, EXPERTS)),
            dma((len(SUM_GROUPS),)),
            dma((len(SUM_GROUPS),)),
            dma((len(SUM_GROUPS),)),
            dma((len(SUM_GROUPS),)),
            dma((EXPERTS, 3, 3, 3)),
            dma((EXPERTS, 3, 3, 3)),
            dma((4,)),
            dma((4,)),
            dma(()),
            dma(()),
        ],
        compiler_params=pltpu.CompilerParams(
            collective_id=0, has_side_effects=True, vmem_limit_bytes=63 * 2**20
        ),
    )(
        master.reshape(rows),
        second.reshape(rows),
        weight.T,
        gain.reshape(1, 128),
    )


def shards(master_down, second_down, router_weight, router_gain):
    final, scale, serve = exchange(master_down, second_down, router_weight, router_gain)
    return final.reshape(EXPERTS, TILES * 8, GROUP * 128), scale, serve.T


def solution(mesh):
    return jax.shard_map(
        shards,
        mesh=mesh,
        in_specs=(P("ep", None, "fsdp"), P("ep", None, "fsdp"), P("fsdp", "ep"), P("fsdp")),
        out_specs=(P("ep", "fsdp", None), P("ep", "fsdp"), P()),
        check_vma=False,
    )
```

```python
import functools

import jax
import jax.numpy as jnp
from jax import lax
from jax.experimental import pallas as pl
from jax.experimental.pallas import tpu as pltpu
from jax.sharding import PartitionSpec as P

MESH = pl.DeviceIdType.MESH

SIZES = {"z": 4, "y": 2, "x": 4}
STRIDES = {"z": 8, "y": 4, "x": 1}
GROUP = 32
EXPERTS = 4
TILES = 25
UNROLL = 8
SUM_GROUPS = ((0,), (1, 2, 3))


def place_of(e):
    g = next(i for i, group in enumerate(SUM_GROUPS) if e in group)
    return g, SUM_GROUPS[g].index(e)


PARTS = (("xyz", 0, 9), ("yzx", 9, 8), ("zxy", 17, 8))


def coords(index):
    return {"z": index // 8, "y": (index // 4) % 2, "x": index % 4}


def moved(at, offset, sign):
    return sum(
        lax.rem(at[dim] + sign * offset[dim] + SIZES[dim], SIZES[dim]) * STRIDES[dim] for dim in "zyx"
    )


def along(dim, step):
    return {other: step if other == dim else 0 for other in "zyx"}


def places():
    lane = lax.broadcasted_iota(jnp.int32, (8, 128), 1)
    row = lax.broadcasted_iota(jnp.int32, (8, 128), 0)
    return lane - lax.rem(row, 4) * 32


def kernel(
    master,
    second,
    weight,
    gain,
    final,
    scale,
    serve,
    merged,
    change,
    buf0,
    buf1,
    buf2,
    sums_out0,
    sums_out1,
    sums_in0,
    sums_in1,
    inverse0,
    inverse1,
    scales,
    columns,
    load_sem,
    sums_send,
    sums_recv,
    inv_send,
    inv_recv,
    part_send,
    part_recv,
    ep_send,
    ep_recv,
    router_send,
    router_recv,
):
    bufs = (buf0, buf1, buf2)
    sums_out = (sums_out0, sums_out1)
    sums_in = (sums_in0, sums_in1)
    inverse = (inverse0, inverse1)
    me = lax.axis_index("fsdp")
    ep = lax.axis_index("ep")
    at = coords(me)

    barrier = pltpu.get_barrier_semaphore()

    def greet(r, _):
        pl.semaphore_signal(
            barrier, inc=1, device_id={"fsdp": moved(at, coords(r), 1)}, device_id_type=MESH
        )
        return _

    lax.fori_loop(1, GROUP, greet, 0)
    for k in range(1, 4):
        pl.semaphore_signal(
            barrier, inc=1, device_id={"ep": lax.rem(ep + k, 4)}, device_id_type=MESH
        )

    def loads(e):
        return (
            pltpu.make_async_copy(master.at[e], merged.at[e], load_sem.at[0, e]),
            pltpu.make_async_copy(second.at[e], change.at[e], load_sem.at[1, e]),
        )

    for e in range(EXPERTS):
        for copy in loads(e):
            copy.start()

    columns[0] = weight[...] * gain[...]

    def merged_rows(e, index):
        rows = pl.ds(index * TILES, TILES)
        return merged[e, rows] + change[e, rows].astype(jnp.float32)

    def add_up(e):
        for copy in loads(e):
            copy.wait()
        g, i = place_of(e)

        def some(step, _):
            key = places()
            packed = []
            for u in range(UNROLL):
                value = merged_rows(e, moved(at, coords(step * UNROLL + u), 1))
                sums = jnp.sum(value * value, axis=2, keepdims=True)
                acc = jnp.zeros((8, 128), jnp.float32)
                for j in range(TILES):
                    acc = jnp.where(key == j, sums[j], acc)
                packed.append(acc)
            for u, acc in enumerate(packed):
                r = step * UNROLL + u
                sums_out[g][r, i, 0:1] = jnp.sum(acc[0:4], axis=0, keepdims=True)
                sums_out[g][r, i, 1:2] = jnp.sum(acc[4:8], axis=0, keepdims=True)
            return _

        lax.fori_loop(0, GROUP // UNROLL, some, 0)

    def sums_copy(g, r):
        return pltpu.make_async_remote_copy(
            src_ref=sums_out[g].at[r],
            dst_ref=sums_in[g].at[r],
            send_sem=sums_send.at[g],
            recv_sem=sums_recv.at[g],
            device_id={"fsdp": moved(at, coords(r), 1)},
            device_id_type=MESH,
        )

    def inv_copy(g, r):
        return pltpu.make_async_remote_copy(
            src_ref=inverse[g].at[0],
            dst_ref=inverse[g].at[r],
            send_sem=inv_send.at[g],
            recv_sem=inv_recv.at[g],
            device_id={"fsdp": moved(at, coords(r), 1)},
            device_id_type=MESH,
        )

    def start_all(copy, g):
        def one(r, _):
            copy(g, r).start()
            return _

        lax.fori_loop(1, GROUP, one, 0)

    def wait_bytes(ref, sem):
        pltpu.make_async_copy(ref, ref, sem).wait()

    def others_of(ref):
        return ref.at[pl.ds(1, GROUP - 1)]

    def send_sums(g):
        sums_in[g][0] = sums_out[g][0]
        start_all(sums_copy, g)

    def send_inverse(g):
        wait_bytes(others_of(sums_in[g]), sums_recv.at[g])
        for i, e in enumerate(SUM_GROUPS[g]):
            root = jnp.sqrt(jnp.sum(sums_in[g][:, i], axis=0))
            scales[e] = root
            inverse[g][0, i] = 1.0 / root
        start_all(inv_copy, g)

    def normalise(e):
        g, i = place_of(e)
        if i == 0:
            wait_bytes(others_of(inverse[g]), inv_recv.at[g])

        def some(step, _):
            key = places()
            factors = []
            for u in range(UNROLL):
                offset = coords(step * UNROLL + u)
                back = {dim: lax.rem(SIZES[dim] - offset[dim], SIZES[dim]) for dim in "zyx"}
                owner = sum(back[dim] * STRIDES[dim] for dim in "zyx")
                packed = inverse[g][owner, i]
                spread = jnp.concatenate(
                    [jnp.broadcast_to(packed[h : h + 1], (4, 128)) for h in range(2)], axis=0
                )
                factors.append(
                    [
                        jnp.sum(jnp.where(key == j, spread, 0.0), axis=1, keepdims=True)
                        for j in range(TILES)
                    ]
                )
            for u in range(UNROLL):
                offset = coords(step * UNROLL + u)
                value = merged_rows(e, moved(at, offset, 1)) * jnp.stack(factors[u])
                value = value.astype(jnp.bfloat16)
                for buf, (order, first, count) in zip(bufs, PARTS):
                    a, b, c = order
                    one_slot = lax.rem(offset[a] + SIZES[a] - 1, SIZES[a])
                    two_slot = lax.rem(offset[b] + SIZES[b] - 1, SIZES[b])
                    buf[e, one_slot, two_slot, offset[c]] = value[first : first + count]
            return _

        lax.fori_loop(0, GROUP // UNROLL, some, 0)

    def first_copies(e, p):
        order, _, _ = PARTS[p]
        n = [SIZES[dim] for dim in order]
        return [
            pltpu.make_async_remote_copy(
                src_ref=bufs[p].at[e, k - 1, pl.ds(0, n[1])],
                dst_ref=bufs[p].at[e, n[0] - 1 + k, pl.ds(0, n[1])],
                send_sem=part_send.at[e, p, 0, k - 1],
                recv_sem=part_recv.at[e, p, 0, k - 1],
                device_id={"fsdp": moved(at, along(order[0], k), 1)},
                device_id_type=MESH,
            )
            for k in ((1, 3, 2) if n[0] == 4 else (1,))
        ]

    def second_copies(e, p):
        order, _, _ = PARTS[p]
        n = [SIZES[dim] for dim in order]
        return [
            pltpu.make_async_remote_copy(
                src_ref=bufs[p].at[e, pl.ds(n[0] - 1, n[0]), k - 1],
                dst_ref=bufs[p].at[e, pl.ds(n[0] - 1, n[0]), n[1] - 1 + k],
                send_sem=part_send.at[e, p, 1, k - 1],
                recv_sem=part_recv.at[e, p, 1, k - 1],
                device_id={"fsdp": moved(at, along(order[1], k), 1)},
                device_id_type=MESH,
            )
            for k in ((1, 3, 2) if n[1] == 4 else (1,))
        ]

    def column(order, i, j):
        offset = {order[0]: i, order[1]: j, order[2]: 0}
        return moved(at, offset, -1)

    def landing(e, p, col):
        _, first, count = PARTS[p]
        return final.at[e, pl.ds(first, count), :, pl.ds(pl.multiple_of(col * 128, 128), 128)]

    def send_third(e, p):
        order, _, _ = PARTS[p]
        n = [SIZES[dim] for dim in order]

        def one(i, k):
            a, b = i // n[1], lax.rem(i, n[1])
            pltpu.make_async_remote_copy(
                src_ref=bufs[p].at[e, n[0] - 1 + a, n[1] - 1 + b, k],
                dst_ref=landing(e, p, column(order, a, b)),
                send_sem=part_send.at[e, p, 2, 0],
                recv_sem=part_recv.at[e, p, 2, 0],
                device_id={"fsdp": moved(at, along(order[2], k), 1)},
                device_id_type=MESH,
            ).start()
            return k

        for k in (1, 3, 2) if n[2] == 4 else (1,):
            lax.fori_loop(0, n[0] * n[1], one, k)

        def keep(i, _):
            a, b = i // n[1], lax.rem(i, n[1])
            col = column(order, a, b)
            first, count = PARTS[p][1:]
            final[e, pl.ds(first, count), :, pl.ds(pl.multiple_of(col * 128, 128), 128)] = bufs[p][
                e, n[0] - 1 + a, n[1] - 1 + b, 0
            ]
            return _

        lax.fori_loop(0, n[0] * n[1], keep, 0)

    def third_bytes(e, p):
        order, first, count = PARTS[p]
        n = [SIZES[dim] for dim in order]
        return final.at[e, pl.ds(first, count), :, pl.ds(0, (n[2] - 1) * n[0] * n[1] * 128)]

    def stage(e, s):
        for p in range(3):
            if s == 0:
                for copy in first_copies(e, p):
                    copy.start()
            elif s == 1:
                for copy in first_copies(e, p):
                    copy.wait_recv()
                for copy in second_copies(e, p):
                    copy.start()
            else:
                for copy in second_copies(e, p):
                    copy.wait_recv()
                send_third(e, p)

    def ep_copy(k):
        return pltpu.make_async_remote_copy(
            src_ref=columns.at[0],
            dst_ref=columns.at[k],
            send_sem=ep_send.at[k],
            recv_sem=ep_recv.at[k],
            device_id={"ep": lax.rem(ep + k, 4)},
            device_id_type=MESH,
        )

    def router_ref():
        return serve.at[:, pl.ds(pl.multiple_of(me * 128, 128), 128)]

    def router_copy(_, r):
        return pltpu.make_async_remote_copy(
            src_ref=router_ref(),
            dst_ref=router_ref(),
            send_sem=router_send,
            recv_sem=router_recv,
            device_id={"fsdp": moved(at, coords(r), 1)},
            device_id_type=MESH,
        )

    def send_router():
        for k in range(1, 4):
            ep_copy(k).wait_recv()
        rows = jnp.concatenate([columns[lax.rem(ep + 4 - i, 4)] for i in range(4)], axis=0)
        serve[:, pl.ds(pl.multiple_of(me * 128, 128), 128)] = rows.astype(jnp.bfloat16)
        start_all(router_copy, 0)

    add_up(0)
    pl.semaphore_wait(barrier, GROUP - 1 + 3)
    send_sums(0)
    for k in range(1, 4):
        ep_copy(k).start()
    for e in SUM_GROUPS[1]:
        add_up(e)
    send_sums(1)
    send_inverse(0)
    send_router()
    send_inverse(1)
    normalise(0)
    stage(0, 0)
    normalise(1)
    stage(1, 0)
    stage(0, 1)
    normalise(2)
    stage(2, 0)
    stage(1, 1)
    stage(0, 2)
    normalise(3)
    stage(3, 0)
    stage(2, 1)
    stage(1, 2)

    def order_of(index):
        source = lax.broadcasted_iota(jnp.int32, (128, 256), 0)
        target = lax.broadcasted_iota(jnp.int32, (128, 256), 1)
        place = lax.rem(source, 32) * 8 + index * 4 + source // 32
        return jnp.where((place == target) & (lax.rem(source, 32) < TILES), 1.0, 0.0)

    in_rows = sum(
        jnp.dot(
            scales[:, index],
            order_of(index),
            precision=lax.Precision.HIGHEST,
            preferred_element_type=jnp.float32,
        )
        for index in range(2)
    )
    scale[...] = in_rows[:, 0 : TILES * 8]

    stage(3, 1)
    stage(2, 2)
    stage(3, 2)

    for g in range(len(SUM_GROUPS)):
        wait_bytes(others_of(sums_out[g]), sums_send.at[g])
        wait_bytes(others_of(inverse[g]), inv_send.at[g])
    for e in range(EXPERTS):
        for p in range(3):
            for copy in first_copies(e, p) + second_copies(e, p):
                copy.wait_send()
            wait_bytes(third_bytes(e, p), part_send.at[e, p, 2, 0])
            wait_bytes(third_bytes(e, p), part_recv.at[e, p, 2, 0])
    for k in range(1, 4):
        ep_copy(k).wait_send()
    others = serve.at[:, pl.ds(0, (GROUP - 1) * 128)]
    wait_bytes(others, router_send)
    wait_bytes(others, router_recv)


def exchange(master, second, weight, gain):
    vmem = pl.BlockSpec(memory_space=pltpu.VMEM)
    hbm = pl.BlockSpec(memory_space=pltpu.HBM)
    rows = EXPERTS, GROUP * TILES, 8, 128
    part_bufs = []
    for order, _, count in PARTS:
        a, b, c = (SIZES[dim] for dim in order)
        part_bufs.append(
            pltpu.VMEM((EXPERTS, 2 * a - 1, 2 * b - 1, c, count, 8, 128), jnp.bfloat16)
        )
    dma = pltpu.SemaphoreType.DMA
    return pl.pallas_call(
        kernel,
        name="exchange",
        out_shape=(
            pltpu.VMEM((EXPERTS, TILES, 8, GROUP * 128), jnp.bfloat16),
            pltpu.VMEM((EXPERTS, TILES * 8), jnp.float32),
            pltpu.VMEM((16, GROUP * 128), jnp.bfloat16),
        ),
        in_specs=[hbm, hbm, vmem, vmem],
        out_specs=(vmem, vmem, vmem),
        scratch_shapes=[
            pltpu.VMEM(rows, jnp.float32),
            pltpu.VMEM(rows, jnp.bfloat16),
            *part_bufs,
            *(
                pltpu.VMEM((GROUP, len(group), 2, 128), jnp.float32)
                for group in SUM_GROUPS + SUM_GROUPS + SUM_GROUPS
            ),
            pltpu.VMEM((EXPERTS, 2, 128), jnp.float32),
            pltpu.VMEM((4, 4, 128), jnp.float32),
            dma((2, EXPERTS)),
            dma((len(SUM_GROUPS),)),
            dma((len(SUM_GROUPS),)),
            dma((len(SUM_GROUPS),)),
            dma((len(SUM_GROUPS),)),
            dma((EXPERTS, 3, 3, 3)),
            dma((EXPERTS, 3, 3, 3)),
            dma((4,)),
            dma((4,)),
            dma(()),
            dma(()),
        ],
        compiler_params=pltpu.CompilerParams(
            collective_id=0, has_side_effects=True, vmem_limit_bytes=48 * 2**20
        ),
    )(
        master.reshape(rows),
        second.reshape(rows),
        weight.T,
        gain.reshape(1, 128),
    )


def write_out(final, scale, serve, final_out, scale_out, serve_out, sem):
    copies = [
        pltpu.make_async_copy(final.at[e], final_out.at[e], sem.at[e]) for e in range(EXPERTS)
    ]
    copies.append(pltpu.make_async_copy(serve, serve_out, sem.at[EXPERTS]))
    copies.append(pltpu.make_async_copy(scale, scale_out, sem.at[EXPERTS + 1]))
    for copy in copies:
        copy.start()
    for copy in copies:
        copy.wait()


def written(final, scale, serve):
    vmem = pl.BlockSpec(memory_space=pltpu.VMEM)
    hbm = pl.BlockSpec(memory_space=pltpu.HBM)
    return pl.pallas_call(
        write_out,
        name="write_out",
        out_shape=tuple(
            jax.ShapeDtypeStruct(value.shape, value.dtype) for value in (final, scale, serve)
        ),
        in_specs=[vmem] * 3,
        out_specs=(hbm,) * 3,
        scratch_shapes=[pltpu.SemaphoreType.DMA((EXPERTS + 2,))],
        compiler_params=pltpu.CompilerParams(vmem_limit_bytes=16 * 2**20),
    )(final, scale, serve)


def shards(master_down, second_down, router_weight, router_gain):
    final, scale, serve = written(
        *exchange(master_down, second_down, router_weight, router_gain)
    )
    return final.reshape(EXPERTS, TILES * 8, GROUP * 128), scale, serve.T


def solution(mesh):
    return jax.shard_map(
        shards,
        mesh=mesh,
        in_specs=(P("ep", None, "fsdp"), P("ep", None, "fsdp"), P("fsdp", "ep"), P("fsdp")),
        out_specs=(P("ep", "fsdp", None), P("ep", "fsdp"), P()),
        check_vma=False,
    )
```

```python
import functools

import jax
import jax.numpy as jnp
from jax import lax
from jax.experimental import pallas as pl
from jax.experimental.pallas import tpu as pltpu
from jax.sharding import PartitionSpec as P

MESH = pl.DeviceIdType.MESH

SIZES = {"z": 4, "y": 2, "x": 4}
STRIDES = {"z": 8, "y": 4, "x": 1}
GROUP = 32
EXPERTS = 4
TILES = 25
UNROLL = 8

SUM_ORDERS = ("xyz", "xyz", "yzx", "zxy")

PARTS = (("xyz", 0, 9), ("yzx", 9, 8), ("zxy", 17, 8))


def coords(index):
    return {"z": index // 8, "y": (index // 4) % 2, "x": index % 4}


def moved(at, offset, sign):
    return sum(
        lax.rem(at[dim] + sign * offset[dim] + SIZES[dim], SIZES[dim]) * STRIDES[dim] for dim in "zyx"
    )


def along(dim, step):
    return {other: step if other == dim else 0 for other in "zyx"}


def places():
    lane = lax.broadcasted_iota(jnp.int32, (8, 128), 1)
    row = lax.broadcasted_iota(jnp.int32, (8, 128), 0)
    return lane - lax.rem(row, 4) * 32


def kernel(
    master,
    second,
    weight,
    gain,
    final,
    scale,
    serve,
    merged,
    change,
    buf0,
    buf1,
    buf2,
    sums,
    sums_in,
    inverse,
    scales,
    columns,
    load_sem,
    sums_send,
    sums_recv,
    part_send,
    part_recv,
    ep_send,
    ep_recv,
    router_send,
    router_recv,
):
    bufs = (buf0, buf1, buf2)
    me = lax.axis_index("fsdp")
    ep = lax.axis_index("ep")
    at = coords(me)

    barrier = pltpu.get_barrier_semaphore()

    for dim in "zyx":
        for k in range(1, SIZES[dim]):
            pl.semaphore_signal(
                barrier,
                inc=1,
                device_id={"fsdp": moved(at, along(dim, k), 1)},
                device_id_type=MESH,
            )
    for k in range(1, 4):
        pl.semaphore_signal(
            barrier, inc=1, device_id={"ep": lax.rem(ep + k, 4)}, device_id_type=MESH
        )

    def loads(e):
        return (
            pltpu.make_async_copy(master.at[e], merged.at[e], load_sem.at[0, e]),
            pltpu.make_async_copy(second.at[e], change.at[e], load_sem.at[1, e]),
        )

    for e in range(EXPERTS):
        for copy in loads(e):
            copy.start()

    columns[0] = weight[...] * gain[...]

    def merged_rows(e, index):
        rows = pl.ds(index * TILES, TILES)
        return merged[e, rows] + change[e, rows].astype(jnp.float32)

    def add_up(e):
        for copy in loads(e):
            copy.wait()

        def some(step, _):
            key = places()
            packed = []
            for u in range(UNROLL):
                value = merged_rows(e, step * UNROLL + u)
                row_sums = jnp.sum(value * value, axis=2, keepdims=True)
                acc = jnp.zeros((8, 128), jnp.float32)
                for j in range(TILES):
                    acc = jnp.where(key == j, row_sums[j], acc)
                packed.append(acc)
            for u, acc in enumerate(packed):
                for h in range(2):
                    row = 2 * (u % 4) + h
                    sums[e, 0, step * (UNROLL // 4) + u // 4, row : row + 1] = jnp.sum(
                        acc[4 * h : 4 * h + 4], axis=0, keepdims=True
                    )
            return _

        lax.fori_loop(0, GROUP // UNROLL, some, 0)

    def wait_bytes(ref, sem):
        pltpu.make_async_copy(ref, ref, sem).wait()

    def arrivals(e, s):
        sizes = [SIZES[dim] - 1 for dim in SUM_ORDERS[e]]
        return sums_in.at[e, pl.ds(sum(sizes[:s]), sizes[s])]

    def send_sums(e, s):
        dim = SUM_ORDERS[e][s] if s < 3 else None
        if s:
            came = arrivals(e, s - 1)
            wait_bytes(came, sums_recv.at[e, s - 1])
            total = sums[e, s - 1]
            for k in range(came.shape[0]):
                total = total + came[k]
            sums[e, s] = total
        if dim is None:
            root = jnp.sqrt(total)
            inverse[e] = 1.0 / root
            index = lax.broadcasted_iota(jnp.int32, root.shape, 0) * 4
            index = index + lax.broadcasted_iota(jnp.int32, root.shape, 1) // 2
            mine = jnp.sum(jnp.where(index == me, root, 0.0), axis=0)
            row = lax.rem(lax.broadcasted_iota(jnp.int32, mine.shape, 0), 2)
            for h in range(2):
                scales[e, h : h + 1] = jnp.sum(
                    jnp.where(row == h, mine, 0.0), axis=0, keepdims=True
                )
            return
        for k in range(1, SIZES[dim]):
            pltpu.make_async_remote_copy(
                src_ref=sums.at[e, s],
                dst_ref=arrivals(e, s).at[k - 1],
                send_sem=sums_send.at[e, s],
                recv_sem=sums_recv.at[e, s],
                device_id={"fsdp": moved(at, along(dim, k), 1)},
                device_id_type=MESH,
            ).start()

    def normalise(e):
        def some(step, _):
            key = places()
            factors = []
            for u in range(UNROLL):
                row = 2 * (u % 4)
                packed = inverse[e, step * (UNROLL // 4) + u // 4, row : row + 2]
                spread = jnp.concatenate(
                    [jnp.broadcast_to(packed[h : h + 1], (4, 128)) for h in range(2)], axis=0
                )
                factors.append(
                    [
                        jnp.sum(jnp.where(key == j, spread, 0.0), axis=1, keepdims=True)
                        for j in range(TILES)
                    ]
                )
            for u in range(UNROLL):
                owner = step * UNROLL + u
                there = coords(owner)
                offset = {dim: lax.rem(there[dim] - at[dim] + SIZES[dim], SIZES[dim]) for dim in "zyx"}
                value = (merged_rows(e, owner) * jnp.stack(factors[u])).astype(jnp.bfloat16)
                for buf, (order, first, count) in zip(bufs, PARTS):
                    a, b, c = order
                    one_slot = lax.rem(offset[a] + SIZES[a] - 1, SIZES[a])
                    two_slot = lax.rem(offset[b] + SIZES[b] - 1, SIZES[b])
                    buf[e, one_slot, two_slot, offset[c]] = value[first : first + count]
            return _

        lax.fori_loop(0, GROUP // UNROLL, some, 0)

    def first_copies(e, p):
        order, _, _ = PARTS[p]
        n = [SIZES[dim] for dim in order]
        return [
            pltpu.make_async_remote_copy(
                src_ref=bufs[p].at[e, k - 1, pl.ds(0, n[1])],
                dst_ref=bufs[p].at[e, n[0] - 1 + k, pl.ds(0, n[1])],
                send_sem=part_send.at[e, p, 0, k - 1],
                recv_sem=part_recv.at[e, p, 0, k - 1],
                device_id={"fsdp": moved(at, along(order[0], k), 1)},
                device_id_type=MESH,
            )
            for k in ((2, 1, 3) if n[0] == 4 else (1,))
        ]

    def second_copies(e, p):
        order, _, _ = PARTS[p]
        n = [SIZES[dim] for dim in order]
        return [
            pltpu.make_async_remote_copy(
                src_ref=bufs[p].at[e, pl.ds(n[0] - 1, n[0]), k - 1],
                dst_ref=bufs[p].at[e, pl.ds(n[0] - 1, n[0]), n[1] - 1 + k],
                send_sem=part_send.at[e, p, 1, k - 1],
                recv_sem=part_recv.at[e, p, 1, k - 1],
                device_id={"fsdp": moved(at, along(order[1], k), 1)},
                device_id_type=MESH,
            )
            for k in ((2, 1, 3) if n[1] == 4 else (1,))
        ]

    def column(order, i, j):
        offset = {order[0]: i, order[1]: j, order[2]: 0}
        return moved(at, offset, -1)

    def landing(e, p, col):
        _, first, count = PARTS[p]
        return final.at[e, pl.ds(first, count), :, pl.ds(pl.multiple_of(col * 128, 128), 128)]

    def send_third(e, p):
        order, _, _ = PARTS[p]
        n = [SIZES[dim] for dim in order]

        def one(i, k):
            a, b = i // n[1], lax.rem(i, n[1])
            pltpu.make_async_remote_copy(
                src_ref=bufs[p].at[e, n[0] - 1 + a, n[1] - 1 + b, k],
                dst_ref=landing(e, p, column(order, a, b)),
                send_sem=part_send.at[e, p, 2, 0],
                recv_sem=part_recv.at[e, p, 2, 0],
                device_id={"fsdp": moved(at, along(order[2], k), 1)},
                device_id_type=MESH,
            ).start()
            return k

        for k in (2, 1, 3) if n[2] == 4 else (1,):
            lax.fori_loop(0, n[0] * n[1], one, k)

        def keep(i, _):
            a, b = i // n[1], lax.rem(i, n[1])
            col = column(order, a, b)
            first, count = PARTS[p][1:]
            final[e, pl.ds(first, count), :, pl.ds(pl.multiple_of(col * 128, 128), 128)] = bufs[p][
                e, n[0] - 1 + a, n[1] - 1 + b, 0
            ]
            return _

        lax.fori_loop(0, n[0] * n[1], keep, 0)

    def third_bytes(e, p):
        order, first, count = PARTS[p]
        n = [SIZES[dim] for dim in order]
        return final.at[e, pl.ds(first, count), :, pl.ds(0, (n[2] - 1) * n[0] * n[1] * 128)]

    def stage(e, s):
        for p in range(3):
            if s == 0:
                for copy in first_copies(e, p):
                    copy.start()
            elif s == 1:
                for copy in first_copies(e, p):
                    copy.wait_recv()
                for copy in second_copies(e, p):
                    copy.start()
            else:
                for copy in second_copies(e, p):
                    copy.wait_recv()
                send_third(e, p)

    def ep_copy(k):
        return pltpu.make_async_remote_copy(
            src_ref=columns.at[0],
            dst_ref=columns.at[k],
            send_sem=ep_send.at[k],
            recv_sem=ep_recv.at[k],
            device_id={"ep": lax.rem(ep + k, 4)},
            device_id_type=MESH,
        )

    spans = ((me, 1, "x"), (me // 4 * 4, 4, "y"), (me // 8 * 8, 8, "z"))

    def router_copies(s):
        start, count, dim = spans[s]
        span = serve.at[:, pl.ds(pl.multiple_of(start * 128, 128), count * 128)]
        return [
            pltpu.make_async_remote_copy(
                src_ref=span,
                dst_ref=span,
                send_sem=router_send.at[s, k - 1],
                recv_sem=router_recv.at[s, k - 1],
                device_id={"fsdp": moved(at, along(dim, k), 1)},
                device_id_type=MESH,
            )
            for k in range(1, SIZES[dim])
        ]

    def send_router(s):
        if s == 0:
            for k in range(1, 4):
                ep_copy(k).wait_recv()
            rows = jnp.concatenate([columns[lax.rem(ep + 4 - i, 4)] for i in range(4)], axis=0)
            serve[:, pl.ds(pl.multiple_of(me * 128, 128), 128)] = rows.astype(jnp.bfloat16)
        else:
            for copy in router_copies(s - 1):
                copy.wait_recv()
        for copy in router_copies(s):
            copy.start()

    add_up(0)
    pl.semaphore_wait(barrier, 10)
    send_sums(0, 0)
    for k in range(1, 4):
        ep_copy(k).start()
    add_up(1)
    send_sums(1, 0)
    add_up(2)
    send_sums(2, 0)
    send_sums(0, 1)
    add_up(3)
    send_sums(3, 0)
    send_sums(1, 1)
    send_sums(0, 2)
    send_sums(2, 1)
    send_sums(3, 1)
    send_router(0)
    send_sums(1, 2)
    send_sums(0, 3)
    normalise(0)
    send_sums(2, 2)
    send_sums(3, 2)
    stage(0, 0)
    send_sums(1, 3)
    normalise(1)
    stage(1, 0)
    send_router(1)
    stage(0, 1)
    send_sums(2, 3)
    normalise(2)
    stage(2, 0)
    stage(1, 1)
    stage(0, 2)
    send_router(2)
    send_sums(3, 3)
    normalise(3)
    stage(3, 0)
    stage(2, 1)
    stage(1, 2)

    def order_of(index):
        source = lax.broadcasted_iota(jnp.int32, (128, 256), 0)
        target = lax.broadcasted_iota(jnp.int32, (128, 256), 1)
        place = lax.rem(source, 32) * 8 + index * 4 + source // 32
        return jnp.where((place == target) & (lax.rem(source, 32) < TILES), 1.0, 0.0)

    in_rows = sum(
        jnp.dot(
            scales[:, index],
            order_of(index),
            precision=lax.Precision.HIGHEST,
            preferred_element_type=jnp.float32,
        )
        for index in range(2)
    )
    scale[...] = in_rows[:, 0 : TILES * 8]

    stage(3, 1)
    stage(2, 2)
    stage(3, 2)

    for e in range(EXPERTS):
        for s in range(3):
            wait_bytes(arrivals(e, s), sums_send.at[e, s])
    for e in range(EXPERTS):
        for p in range(3):
            for copy in first_copies(e, p) + second_copies(e, p):
                copy.wait_send()
            wait_bytes(third_bytes(e, p), part_send.at[e, p, 2, 0])
            wait_bytes(third_bytes(e, p), part_recv.at[e, p, 2, 0])
    for k in range(1, 4):
        ep_copy(k).wait_send()
    for s in range(3):
        for copy in router_copies(s):
            copy.wait_send()
            if s == 2:
                copy.wait_recv()


def exchange(master, second, weight, gain):
    vmem = pl.BlockSpec(memory_space=pltpu.VMEM)
    hbm = pl.BlockSpec(memory_space=pltpu.HBM)
    rows = EXPERTS, GROUP * TILES, 8, 128
    part_bufs = []
    for order, _, count in PARTS:
        a, b, c = (SIZES[dim] for dim in order)
        part_bufs.append(
            pltpu.VMEM((EXPERTS, 2 * a - 1, 2 * b - 1, c, count, 8, 128), jnp.bfloat16)
        )
    dma = pltpu.SemaphoreType.DMA
    return pl.pallas_call(
        kernel,
        name="exchange",
        out_shape=(
            pltpu.VMEM((EXPERTS, TILES, 8, GROUP * 128), jnp.bfloat16),
            pltpu.VMEM((EXPERTS, TILES * 8), jnp.float32),
            pltpu.VMEM((16, GROUP * 128), jnp.bfloat16),
        ),
        in_specs=[hbm, hbm, vmem, vmem],
        out_specs=(vmem, vmem, vmem),
        scratch_shapes=[
            pltpu.VMEM(rows, jnp.float32),
            pltpu.VMEM(rows, jnp.bfloat16),
            *part_bufs,
            pltpu.VMEM((EXPERTS, 4, GROUP // 4, 8, 128), jnp.float32),
            pltpu.VMEM((EXPERTS, 7, GROUP // 4, 8, 128), jnp.float32),
            pltpu.VMEM((EXPERTS, GROUP // 4, 8, 128), jnp.float32),
            pltpu.VMEM((EXPERTS, 2, 128), jnp.float32),
            pltpu.VMEM((4, 4, 128), jnp.float32),
            dma((2, EXPERTS)),
            dma((EXPERTS, 3)),
            dma((EXPERTS, 3)),
            dma((EXPERTS, 3, 3, 3)),
            dma((EXPERTS, 3, 3, 3)),
            dma((4,)),
            dma((4,)),
            dma((3, 3)),
            dma((3, 3)),
        ],
        compiler_params=pltpu.CompilerParams(
            collective_id=0, has_side_effects=True, vmem_limit_bytes=48 * 2**20
        ),
    )(
        master.reshape(rows),
        second.reshape(rows),
        weight.T,
        gain.reshape(1, 128),
    )


def write_out(final, scale, serve, final_out, scale_out, serve_out, sem):
    copies = [
        pltpu.make_async_copy(final.at[e], final_out.at[e], sem.at[e]) for e in range(EXPERTS)
    ]
    copies.append(pltpu.make_async_copy(serve, serve_out, sem.at[EXPERTS]))
    copies.append(pltpu.make_async_copy(scale, scale_out, sem.at[EXPERTS + 1]))
    for copy in copies:
        copy.start()
    for copy in copies:
        copy.wait()


def written(final, scale, serve):
    vmem = pl.BlockSpec(memory_space=pltpu.VMEM)
    hbm = pl.BlockSpec(memory_space=pltpu.HBM)
    return pl.pallas_call(
        write_out,
        name="write_out",
        out_shape=tuple(
            jax.ShapeDtypeStruct(value.shape, value.dtype) for value in (final, scale, serve)
        ),
        in_specs=[vmem] * 3,
        out_specs=(hbm,) * 3,
        scratch_shapes=[pltpu.SemaphoreType.DMA((EXPERTS + 2,))],
        compiler_params=pltpu.CompilerParams(vmem_limit_bytes=16 * 2**20),
    )(final, scale, serve)


def shards(master_down, second_down, router_weight, router_gain):
    final, scale, serve = written(
        *exchange(master_down, second_down, router_weight, router_gain)
    )
    return final.reshape(EXPERTS, TILES * 8, GROUP * 128), scale, serve.T


def solution(mesh):
    return jax.shard_map(
        shards,
        mesh=mesh,
        in_specs=(P("ep", None, "fsdp"), P("ep", None, "fsdp"), P("fsdp", "ep"), P("fsdp")),
        out_specs=(P("ep", "fsdp", None), P("ep", "fsdp"), P()),
        check_vma=False,
    )
```

```python
import functools

import jax
import jax.numpy as jnp
from jax import lax
from jax.experimental import pallas as pl
from jax.experimental.pallas import tpu as pltpu
from jax.sharding import PartitionSpec as P

MESH = pl.DeviceIdType.MESH

SIZES = {"z": 4, "y": 2, "x": 4}
STRIDES = {"z": 8, "y": 4, "x": 1}
GROUP = 32
EXPERTS = 4
TILES = 25
UNROLL = 16

SUM_ORDERS = ("xyz", "xyz", "yzx", "zxy")

PARTS = (("xyz", 0, 9), ("yzx", 9, 8), ("zxy", 17, 8))


def coords(index):
    return {"z": index // 8, "y": (index // 4) % 2, "x": index % 4}


def moved(at, offset, sign):
    return sum(
        lax.rem(at[dim] + sign * offset[dim] + SIZES[dim], SIZES[dim]) * STRIDES[dim] for dim in "zyx"
    )


def along(dim, step):
    return {other: step if other == dim else 0 for other in "zyx"}


def places():
    lane = lax.broadcasted_iota(jnp.int32, (8, 128), 1)
    row = lax.broadcasted_iota(jnp.int32, (8, 128), 0)
    return lane - lax.rem(row, 4) * 32


def kernel(
    master,
    second,
    weight,
    gain,
    final,
    scale,
    serve,
    merged,
    change,
    buf0,
    buf1,
    buf2,
    sums,
    sums_in,
    inverse,
    scales,
    columns,
    load_sem,
    sums_send,
    sums_recv,
    part_send,
    part_recv,
    ep_send,
    ep_recv,
    router_send,
    router_recv,
):
    bufs = (buf0, buf1, buf2)
    me = lax.axis_index("fsdp")
    ep = lax.axis_index("ep")
    at = coords(me)

    barrier = pltpu.get_barrier_semaphore()

    for dim in "zyx":
        for k in range(1, SIZES[dim]):
            pl.semaphore_signal(
                barrier,
                inc=1,
                device_id={"fsdp": moved(at, along(dim, k), 1)},
                device_id_type=MESH,
            )
    for k in range(1, 4):
        pl.semaphore_signal(
            barrier, inc=1, device_id={"ep": lax.rem(ep + k, 4)}, device_id_type=MESH
        )

    def loads(e):
        return (
            pltpu.make_async_copy(master.at[e], merged.at[e], load_sem.at[0, e]),
            pltpu.make_async_copy(second.at[e], change.at[e], load_sem.at[1, e]),
        )

    for e in range(EXPERTS):
        for copy in loads(e):
            copy.start()

    columns[0] = weight[...] * gain[...]

    def merged_rows(e, index):
        rows = pl.ds(index * TILES, TILES)
        return merged[e, rows] + change[e, rows].astype(jnp.float32)

    def add_up(e):
        for copy in loads(e):
            copy.wait()

        def some(step, _):
            key = places()
            packed = []
            for u in range(UNROLL):
                value = merged_rows(e, step * UNROLL + u)
                row_sums = jnp.sum(value * value, axis=2, keepdims=True)
                acc = jnp.zeros((8, 128), jnp.float32)
                for j in range(TILES):
                    acc = jnp.where(key == j, row_sums[j], acc)
                packed.append(acc)
            for u, acc in enumerate(packed):
                for h in range(2):
                    row = 2 * (u % 4) + h
                    sums[e, 0, step * (UNROLL // 4) + u // 4, row : row + 1] = jnp.sum(
                        acc[4 * h : 4 * h + 4], axis=0, keepdims=True
                    )
            return _

        lax.fori_loop(0, GROUP // UNROLL, some, 0)

    def wait_bytes(ref, sem):
        pltpu.make_async_copy(ref, ref, sem).wait()

    def arrivals(e, s):
        sizes = [SIZES[dim] - 1 for dim in SUM_ORDERS[e]]
        return sums_in.at[e, pl.ds(sum(sizes[:s]), sizes[s])]

    def send_sums(e, s):
        dim = SUM_ORDERS[e][s] if s < 3 else None
        if s:
            came = arrivals(e, s - 1)
            wait_bytes(came, sums_recv.at[e, s - 1])
            total = sums[e, s - 1]
            for k in range(came.shape[0]):
                total = total + came[k]
            sums[e, s] = total
        if dim is None:
            root = jnp.sqrt(total)
            inverse[e] = 1.0 / root
            index = lax.broadcasted_iota(jnp.int32, root.shape, 0) * 4
            index = index + lax.broadcasted_iota(jnp.int32, root.shape, 1) // 2
            mine = jnp.sum(jnp.where(index == me, root, 0.0), axis=0)
            row = lax.rem(lax.broadcasted_iota(jnp.int32, mine.shape, 0), 2)
            for h in range(2):
                scales[e, h : h + 1] = jnp.sum(
                    jnp.where(row == h, mine, 0.0), axis=0, keepdims=True
                )
            return
        for k in range(1, SIZES[dim]):
            pltpu.make_async_remote_copy(
                src_ref=sums.at[e, s],
                dst_ref=arrivals(e, s).at[k - 1],
                send_sem=sums_send.at[e, s],
                recv_sem=sums_recv.at[e, s],
                device_id={"fsdp": moved(at, along(dim, k), 1)},
                device_id_type=MESH,
            ).start()

    def normalise(e):
        def some(step, _):
            key = places()
            factors = []
            for u in range(UNROLL):
                row = 2 * (u % 4)
                packed = inverse[e, step * (UNROLL // 4) + u // 4, row : row + 2]
                spread = jnp.concatenate(
                    [jnp.broadcast_to(packed[h : h + 1], (4, 128)) for h in range(2)], axis=0
                )
                factors.append(
                    [
                        jnp.sum(jnp.where(key == j, spread, 0.0), axis=1, keepdims=True)
                        for j in range(TILES)
                    ]
                )
            for u in range(UNROLL):
                owner = step * UNROLL + u
                there = coords(owner)
                offset = {dim: lax.rem(there[dim] - at[dim] + SIZES[dim], SIZES[dim]) for dim in "zyx"}
                value = (merged_rows(e, owner) * jnp.stack(factors[u])).astype(jnp.bfloat16)
                for buf, (order, first, count) in zip(bufs, PARTS):
                    a, b, c = order
                    one_slot = lax.rem(offset[a] + SIZES[a] - 1, SIZES[a])
                    two_slot = lax.rem(offset[b] + SIZES[b] - 1, SIZES[b])
                    buf[e, one_slot, two_slot, offset[c]] = value[first : first + count]
            return _

        lax.fori_loop(0, GROUP // UNROLL, some, 0)

    def first_copies(e, p):
        order, _, _ = PARTS[p]
        n = [SIZES[dim] for dim in order]
        return [
            pltpu.make_async_remote_copy(
                src_ref=bufs[p].at[e, k - 1, pl.ds(0, n[1])],
                dst_ref=bufs[p].at[e, n[0] - 1 + k, pl.ds(0, n[1])],
                send_sem=part_send.at[e, p, 0, k - 1],
                recv_sem=part_recv.at[e, p, 0, k - 1],
                device_id={"fsdp": moved(at, along(order[0], k), 1)},
                device_id_type=MESH,
            )
            for k in ((2, 1, 3) if n[0] == 4 else (1,))
        ]

    def second_copies(e, p):
        order, _, _ = PARTS[p]
        n = [SIZES[dim] for dim in order]
        return [
            pltpu.make_async_remote_copy(
                src_ref=bufs[p].at[e, pl.ds(n[0] - 1, n[0]), k - 1],
                dst_ref=bufs[p].at[e, pl.ds(n[0] - 1, n[0]), n[1] - 1 + k],
                send_sem=part_send.at[e, p, 1, k - 1],
                recv_sem=part_recv.at[e, p, 1, k - 1],
                device_id={"fsdp": moved(at, along(order[1], k), 1)},
                device_id_type=MESH,
            )
            for k in ((2, 1, 3) if n[1] == 4 else (1,))
        ]

    def column(order, i, j):
        offset = {order[0]: i, order[1]: j, order[2]: 0}
        return moved(at, offset, -1)

    def landing(e, p, col):
        _, first, count = PARTS[p]
        return final.at[e, pl.ds(first, count), :, pl.ds(pl.multiple_of(col * 128, 128), 128)]

    def send_third(e, p):
        order, _, _ = PARTS[p]
        n = [SIZES[dim] for dim in order]

        def one(i, k):
            a, b = i // n[1], lax.rem(i, n[1])
            pltpu.make_async_remote_copy(
                src_ref=bufs[p].at[e, n[0] - 1 + a, n[1] - 1 + b, k],
                dst_ref=landing(e, p, column(order, a, b)),
                send_sem=part_send.at[e, p, 2, 0],
                recv_sem=part_recv.at[e, p, 2, 0],
                device_id={"fsdp": moved(at, along(order[2], k), 1)},
                device_id_type=MESH,
            ).start()
            return k

        for k in (2, 1, 3) if n[2] == 4 else (1,):
            lax.fori_loop(0, n[0] * n[1], one, k)

        def keep(i, _):
            a, b = i // n[1], lax.rem(i, n[1])
            col = column(order, a, b)
            first, count = PARTS[p][1:]
            final[e, pl.ds(first, count), :, pl.ds(pl.multiple_of(col * 128, 128), 128)] = bufs[p][
                e, n[0] - 1 + a, n[1] - 1 + b, 0
            ]
            return _

        lax.fori_loop(0, n[0] * n[1], keep, 0)

    def third_bytes(e, p):
        order, first, count = PARTS[p]
        n = [SIZES[dim] for dim in order]
        return final.at[e, pl.ds(first, count), :, pl.ds(0, (n[2] - 1) * n[0] * n[1] * 128)]

    def stage(e, s):
        for p in range(3):
            if s == 0:
                for copy in first_copies(e, p):
                    copy.start()
            elif s == 1:
                for copy in first_copies(e, p):
                    copy.wait_recv()
                for copy in second_copies(e, p):
                    copy.start()
            else:
                for copy in second_copies(e, p):
                    copy.wait_recv()
                send_third(e, p)

    def ep_copy(k):
        return pltpu.make_async_remote_copy(
            src_ref=columns.at[0],
            dst_ref=columns.at[k],
            send_sem=ep_send.at[k],
            recv_sem=ep_recv.at[k],
            device_id={"ep": lax.rem(ep + k, 4)},
            device_id_type=MESH,
        )

    spans = ((me, 1, "x"), (me // 4 * 4, 4, "y"), (me // 8 * 8, 8, "z"))

    def router_copies(s):
        start, count, dim = spans[s]
        span = serve.at[:, pl.ds(pl.multiple_of(start * 128, 128), count * 128)]
        return [
            pltpu.make_async_remote_copy(
                src_ref=span,
                dst_ref=span,
                send_sem=router_send.at[s, k - 1],
                recv_sem=router_recv.at[s, k - 1],
                device_id={"fsdp": moved(at, along(dim, k), 1)},
                device_id_type=MESH,
            )
            for k in range(1, SIZES[dim])
        ]

    def send_router(s):
        if s == 0:
            for k in range(1, 4):
                ep_copy(k).wait_recv()
            rows = jnp.concatenate([columns[lax.rem(ep + 4 - i, 4)] for i in range(4)], axis=0)
            serve[:, pl.ds(pl.multiple_of(me * 128, 128), 128)] = rows.astype(jnp.bfloat16)
        else:
            for copy in router_copies(s - 1):
                copy.wait_recv()
        for copy in router_copies(s):
            copy.start()

    add_up(0)
    pl.semaphore_wait(barrier, 10)
    send_sums(0, 0)
    for k in range(1, 4):
        ep_copy(k).start()
    add_up(1)
    send_sums(1, 0)
    add_up(2)
    send_sums(2, 0)
    send_sums(0, 1)
    add_up(3)
    send_sums(3, 0)
    send_sums(1, 1)
    send_sums(0, 2)
    send_sums(2, 1)
    send_sums(3, 1)
    send_router(0)
    send_sums(1, 2)
    send_sums(0, 3)
    normalise(0)
    stage(0, 0)
    send_sums(2, 2)
    send_sums(3, 2)
    send_sums(1, 3)
    normalise(1)
    stage(1, 0)
    send_router(1)
    stage(0, 1)
    send_sums(2, 3)
    normalise(2)
    stage(2, 0)
    stage(1, 1)
    stage(0, 2)
    send_router(2)
    send_sums(3, 3)
    normalise(3)
    stage(3, 0)
    stage(2, 1)
    stage(1, 2)

    stage(3, 1)
    stage(2, 2)
    stage(3, 2)

    def order_of(index):
        source = lax.broadcasted_iota(jnp.int32, (128, 256), 0)
        target = lax.broadcasted_iota(jnp.int32, (128, 256), 1)
        place = lax.rem(source, 32) * 8 + index * 4 + source // 32
        return jnp.where((place == target) & (lax.rem(source, 32) < TILES), 1.0, 0.0)

    in_rows = sum(
        jnp.dot(
            scales[:, index],
            order_of(index),
            precision=lax.Precision.HIGHEST,
            preferred_element_type=jnp.float32,
        )
        for index in range(2)
    )
    scale[...] = in_rows[:, 0 : TILES * 8]

    for e in range(EXPERTS):
        for s in range(3):
            wait_bytes(arrivals(e, s), sums_send.at[e, s])
    for e in range(EXPERTS):
        for p in range(3):
            for copy in first_copies(e, p) + second_copies(e, p):
                copy.wait_send()
            wait_bytes(third_bytes(e, p), part_send.at[e, p, 2, 0])
            wait_bytes(third_bytes(e, p), part_recv.at[e, p, 2, 0])
    for k in range(1, 4):
        ep_copy(k).wait_send()
    for s in range(3):
        for copy in router_copies(s):
            copy.wait_send()
            if s == 2:
                copy.wait_recv()


def exchange(master, second, weight, gain):
    vmem = pl.BlockSpec(memory_space=pltpu.VMEM)
    hbm = pl.BlockSpec(memory_space=pltpu.HBM)
    rows = EXPERTS, GROUP * TILES, 8, 128
    part_bufs = []
    for order, _, count in PARTS:
        a, b, c = (SIZES[dim] for dim in order)
        part_bufs.append(
            pltpu.VMEM((EXPERTS, 2 * a - 1, 2 * b - 1, c, count, 8, 128), jnp.bfloat16)
        )
    dma = pltpu.SemaphoreType.DMA
    return pl.pallas_call(
        kernel,
        name="exchange",
        out_shape=(
            pltpu.VMEM((EXPERTS, TILES, 8, GROUP * 128), jnp.bfloat16),
            pltpu.VMEM((EXPERTS, TILES * 8), jnp.float32),
            pltpu.VMEM((16, GROUP * 128), jnp.bfloat16),
        ),
        in_specs=[hbm, hbm, vmem, vmem],
        out_specs=(vmem, vmem, vmem),
        scratch_shapes=[
            pltpu.VMEM(rows, jnp.float32),
            pltpu.VMEM(rows, jnp.bfloat16),
            *part_bufs,
            pltpu.VMEM((EXPERTS, 4, GROUP // 4, 8, 128), jnp.float32),
            pltpu.VMEM((EXPERTS, 7, GROUP // 4, 8, 128), jnp.float32),
            pltpu.VMEM((EXPERTS, GROUP // 4, 8, 128), jnp.float32),
            pltpu.VMEM((EXPERTS, 2, 128), jnp.float32),
            pltpu.VMEM((4, 4, 128), jnp.float32),
            dma((2, EXPERTS)),
            dma((EXPERTS, 3)),
            dma((EXPERTS, 3)),
            dma((EXPERTS, 3, 3, 3)),
            dma((EXPERTS, 3, 3, 3)),
            dma((4,)),
            dma((4,)),
            dma((3, 3)),
            dma((3, 3)),
        ],
        compiler_params=pltpu.CompilerParams(
            collective_id=0, has_side_effects=True, vmem_limit_bytes=48 * 2**20
        ),
    )(
        master.reshape(rows),
        second.reshape(rows),
        weight.T,
        gain.reshape(1, 128),
    )


def write_out(final, scale, serve, final_out, scale_out, serve_out, sem):
    copies = [
        pltpu.make_async_copy(final.at[e], final_out.at[e], sem.at[e]) for e in range(EXPERTS)
    ]
    copies.append(pltpu.make_async_copy(serve, serve_out, sem.at[EXPERTS]))
    copies.append(pltpu.make_async_copy(scale, scale_out, sem.at[EXPERTS + 1]))
    for copy in copies:
        copy.start()
    for copy in copies:
        copy.wait()


def written(final, scale, serve):
    vmem = pl.BlockSpec(memory_space=pltpu.VMEM)
    hbm = pl.BlockSpec(memory_space=pltpu.HBM)
    return pl.pallas_call(
        write_out,
        name="write_out",
        out_shape=tuple(
            jax.ShapeDtypeStruct(value.shape, value.dtype) for value in (final, scale, serve)
        ),
        in_specs=[vmem] * 3,
        out_specs=(hbm,) * 3,
        scratch_shapes=[pltpu.SemaphoreType.DMA((EXPERTS + 2,))],
        compiler_params=pltpu.CompilerParams(vmem_limit_bytes=16 * 2**20),
    )(final, scale, serve)


def shards(master_down, second_down, router_weight, router_gain):
    final, scale, serve = written(
        *exchange(master_down, second_down, router_weight, router_gain)
    )
    return final.reshape(EXPERTS, TILES * 8, GROUP * 128), scale, serve.T


def solution(mesh):
    return jax.shard_map(
        shards,
        mesh=mesh,
        in_specs=(P("ep", None, "fsdp"), P("ep", None, "fsdp"), P("fsdp", "ep"), P("fsdp")),
        out_specs=(P("ep", "fsdp", None), P("ep", "fsdp"), P()),
        check_vma=False,
    )
```

```python
import functools

import jax
import jax.numpy as jnp
from jax import lax
from jax.experimental import pallas as pl
from jax.experimental.pallas import tpu as pltpu
from jax.sharding import PartitionSpec as P

MESH = pl.DeviceIdType.MESH

SIZES = {"z": 4, "y": 2, "x": 4}
STRIDES = {"z": 8, "y": 4, "x": 1}
GROUP = 32
EXPERTS = 4
TILES = 25
UNROLL = 16

SUM_ORDERS = ("xyz", "xyz", "yzx", "zxy")

PARTS = (("xyz", 0, 8), ("yzx", 8, 8), ("zxy", 16, 9))


def coords(index):
    return {"z": index // 8, "y": (index // 4) % 2, "x": index % 4}


def moved(at, offset, sign):
    return sum(
        lax.rem(at[dim] + sign * offset[dim] + SIZES[dim], SIZES[dim]) * STRIDES[dim] for dim in "zyx"
    )


def along(dim, step):
    return {other: step if other == dim else 0 for other in "zyx"}


def places():
    lane = lax.broadcasted_iota(jnp.int32, (8, 128), 1)
    row = lax.broadcasted_iota(jnp.int32, (8, 128), 0)
    return lane - lax.rem(row, 4) * 32


def kernel(
    master,
    second,
    weight,
    gain,
    final,
    scale,
    serve,
    merged,
    change,
    buf0,
    buf1,
    buf2,
    sums,
    sums_in,
    inverse,
    scales,
    columns,
    load_sem,
    sums_send,
    sums_recv,
    part_send,
    part_recv,
    ep_send,
    ep_recv,
    router_send,
    router_recv,
):
    bufs = (buf0, buf1, buf2)
    me = lax.axis_index("fsdp")
    ep = lax.axis_index("ep")
    at = coords(me)

    barrier = pltpu.get_barrier_semaphore()

    for dim in "zyx":
        for k in range(1, SIZES[dim]):
            pl.semaphore_signal(
                barrier,
                inc=1,
                device_id={"fsdp": moved(at, along(dim, k), 1)},
                device_id_type=MESH,
            )
    for k in range(1, 4):
        pl.semaphore_signal(
            barrier, inc=1, device_id={"ep": lax.rem(ep + k, 4)}, device_id_type=MESH
        )

    def loads(e):
        return (
            pltpu.make_async_copy(master.at[e], merged.at[e], load_sem.at[0, e]),
            pltpu.make_async_copy(second.at[e], change.at[e], load_sem.at[1, e]),
        )

    for e in range(EXPERTS):
        for copy in loads(e):
            copy.start()

    columns[0] = weight[...] * gain[...]

    def merged_rows(e, index):
        rows = pl.ds(index * TILES, TILES)
        return merged[e, rows] + change[e, rows].astype(jnp.float32)

    def add_up(e):
        for copy in loads(e):
            copy.wait()

        def some(step, _):
            key = places()
            packed = []
            for u in range(UNROLL):
                value = merged_rows(e, step * UNROLL + u)
                row_sums = jnp.sum(value * value, axis=2, keepdims=True)
                acc = jnp.zeros((8, 128), jnp.float32)
                for j in range(TILES):
                    acc = jnp.where(key == j, row_sums[j], acc)
                packed.append(acc)
            for u, acc in enumerate(packed):
                for h in range(2):
                    row = 2 * (u % 4) + h
                    sums[e, 0, step * (UNROLL // 4) + u // 4, row : row + 1] = jnp.sum(
                        acc[4 * h : 4 * h + 4], axis=0, keepdims=True
                    )
            return _

        lax.fori_loop(0, GROUP // UNROLL, some, 0)

    def wait_bytes(ref, sem):
        pltpu.make_async_copy(ref, ref, sem).wait()

    def arrivals(e, s):
        sizes = [SIZES[dim] - 1 for dim in SUM_ORDERS[e]]
        return sums_in.at[e, pl.ds(sum(sizes[:s]), sizes[s])]

    def send_sums(e, s):
        dim = SUM_ORDERS[e][s] if s < 3 else None
        if s:
            came = arrivals(e, s - 1)
            wait_bytes(came, sums_recv.at[e, s - 1])
            total = sums[e, s - 1]
            for k in range(came.shape[0]):
                total = total + came[k]
            sums[e, s] = total
        if dim is None:
            root = jnp.sqrt(total)
            inverse[e] = 1.0 / root
            index = lax.broadcasted_iota(jnp.int32, root.shape, 0) * 4
            index = index + lax.broadcasted_iota(jnp.int32, root.shape, 1) // 2
            mine = jnp.sum(jnp.where(index == me, root, 0.0), axis=0)
            row = lax.rem(lax.broadcasted_iota(jnp.int32, mine.shape, 0), 2)
            for h in range(2):
                scales[e, h : h + 1] = jnp.sum(
                    jnp.where(row == h, mine, 0.0), axis=0, keepdims=True
                )
            return
        for k in range(1, SIZES[dim]):
            pltpu.make_async_remote_copy(
                src_ref=sums.at[e, s],
                dst_ref=arrivals(e, s).at[k - 1],
                send_sem=sums_send.at[e, s],
                recv_sem=sums_recv.at[e, s],
                device_id={"fsdp": moved(at, along(dim, k), 1)},
                device_id_type=MESH,
            ).start()

    def normalise(e):
        def some(step, _):
            key = places()
            factors = []
            for u in range(UNROLL):
                row = 2 * (u % 4)
                packed = inverse[e, step * (UNROLL // 4) + u // 4, row : row + 2]
                spread = jnp.concatenate(
                    [jnp.broadcast_to(packed[h : h + 1], (4, 128)) for h in range(2)], axis=0
                )
                factors.append(
                    [
                        jnp.sum(jnp.where(key == j, spread, 0.0), axis=1, keepdims=True)
                        for j in range(TILES)
                    ]
                )
            for u in range(UNROLL):
                owner = step * UNROLL + u
                there = coords(owner)
                offset = {dim: lax.rem(there[dim] - at[dim] + SIZES[dim], SIZES[dim]) for dim in "zyx"}
                value = (merged_rows(e, owner) * jnp.stack(factors[u])).astype(jnp.bfloat16)
                for buf, (order, first, count) in zip(bufs, PARTS):
                    a, b, c = order
                    one_slot = lax.rem(offset[a] + SIZES[a] - 1, SIZES[a])
                    two_slot = lax.rem(offset[b] + SIZES[b] - 1, SIZES[b])
                    buf[e, one_slot, two_slot, offset[c]] = value[first : first + count]
            return _

        lax.fori_loop(0, GROUP // UNROLL, some, 0)

    def first_copies(e, p):
        order, _, _ = PARTS[p]
        n = [SIZES[dim] for dim in order]
        return [
            pltpu.make_async_remote_copy(
                src_ref=bufs[p].at[e, k - 1, pl.ds(0, n[1])],
                dst_ref=bufs[p].at[e, n[0] - 1 + k, pl.ds(0, n[1])],
                send_sem=part_send.at[e, p, 0, k - 1],
                recv_sem=part_recv.at[e, p, 0, k - 1],
                device_id={"fsdp": moved(at, along(order[0], k), 1)},
                device_id_type=MESH,
            )
            for k in ((2, 1, 3) if n[0] == 4 else (1,))
        ]

    def second_copies(e, p):
        order, _, _ = PARTS[p]
        n = [SIZES[dim] for dim in order]
        return [
            pltpu.make_async_remote_copy(
                src_ref=bufs[p].at[e, pl.ds(n[0] - 1, n[0]), k - 1],
                dst_ref=bufs[p].at[e, pl.ds(n[0] - 1, n[0]), n[1] - 1 + k],
                send_sem=part_send.at[e, p, 1, k - 1],
                recv_sem=part_recv.at[e, p, 1, k - 1],
                device_id={"fsdp": moved(at, along(order[1], k), 1)},
                device_id_type=MESH,
            )
            for k in ((2, 1, 3) if n[1] == 4 else (1,))
        ]

    def column(order, i, j):
        offset = {order[0]: i, order[1]: j, order[2]: 0}
        return moved(at, offset, -1)

    def landing(e, p, col):
        _, first, count = PARTS[p]
        return final.at[e, pl.ds(first, count), :, pl.ds(pl.multiple_of(col * 128, 128), 128)]

    def send_third(e, p):
        order, _, _ = PARTS[p]
        n = [SIZES[dim] for dim in order]

        def one(i, k):
            a, b = i // n[1], lax.rem(i, n[1])
            pltpu.make_async_remote_copy(
                src_ref=bufs[p].at[e, n[0] - 1 + a, n[1] - 1 + b, k],
                dst_ref=landing(e, p, column(order, a, b)),
                send_sem=part_send.at[e, p, 2, 0],
                recv_sem=part_recv.at[e, p, 2, 0],
                device_id={"fsdp": moved(at, along(order[2], k), 1)},
                device_id_type=MESH,
            ).start()
            return k

        for k in (2, 1, 3) if n[2] == 4 else (1,):
            lax.fori_loop(0, n[0] * n[1], one, k)

        def keep(i, _):
            a, b = i // n[1], lax.rem(i, n[1])
            col = column(order, a, b)
            first, count = PARTS[p][1:]
            final[e, pl.ds(first, count), :, pl.ds(pl.multiple_of(col * 128, 128), 128)] = bufs[p][
                e, n[0] - 1 + a, n[1] - 1 + b, 0
            ]
            return _

        lax.fori_loop(0, n[0] * n[1], keep, 0)

    def third_bytes(e, p):
        order, first, count = PARTS[p]
        n = [SIZES[dim] for dim in order]
        return final.at[e, pl.ds(first, count), :, pl.ds(0, (n[2] - 1) * n[0] * n[1] * 128)]

    def stage(e, s):
        for p in range(3):
            if s == 0:
                for copy in first_copies(e, p):
                    copy.start()
            elif s == 1:
                for copy in first_copies(e, p):
                    copy.wait_recv()
                for copy in second_copies(e, p):
                    copy.start()
            else:
                for copy in second_copies(e, p):
                    copy.wait_recv()
                send_third(e, p)

    def ep_copy(k):
        return pltpu.make_async_remote_copy(
            src_ref=columns.at[0],
            dst_ref=columns.at[k],
            send_sem=ep_send.at[k],
            recv_sem=ep_recv.at[k],
            device_id={"ep": lax.rem(ep + k, 4)},
            device_id_type=MESH,
        )

    spans = ((me, 1, "x"), (me // 4 * 4, 4, "y"), (me // 8 * 8, 8, "z"))

    def router_copies(s):
        start, count, dim = spans[s]
        span = serve.at[:, pl.ds(pl.multiple_of(start * 128, 128), count * 128)]
        return [
            pltpu.make_async_remote_copy(
                src_ref=span,
                dst_ref=span,
                send_sem=router_send.at[s, k - 1],
                recv_sem=router_recv.at[s, k - 1],
                device_id={"fsdp": moved(at, along(dim, k), 1)},
                device_id_type=MESH,
            )
            for k in range(1, SIZES[dim])
        ]

    def send_router(s):
        if s == 0:
            for k in range(1, 4):
                ep_copy(k).wait_recv()
            rows = jnp.concatenate([columns[lax.rem(ep + 4 - i, 4)] for i in range(4)], axis=0)
            serve[:, pl.ds(pl.multiple_of(me * 128, 128), 128)] = rows.astype(jnp.bfloat16)
        else:
            for copy in router_copies(s - 1):
                copy.wait_recv()
        for copy in router_copies(s):
            copy.start()

    add_up(0)
    pl.semaphore_wait(barrier, 10)
    send_sums(0, 0)
    for k in range(1, 4):
        ep_copy(k).start()
    add_up(1)
    send_sums(1, 0)
    add_up(2)
    send_sums(2, 0)
    send_sums(0, 1)
    add_up(3)
    send_sums(3, 0)
    send_sums(1, 1)
    send_sums(0, 2)
    send_sums(2, 1)
    send_sums(3, 1)
    send_router(0)
    send_sums(1, 2)
    send_sums(0, 3)
    normalise(0)
    stage(0, 0)
    send_sums(2, 2)
    send_sums(3, 2)
    send_sums(1, 3)
    normalise(1)
    stage(1, 0)
    send_router(1)
    stage(0, 1)
    send_sums(2, 3)
    normalise(2)
    stage(2, 0)
    stage(1, 1)
    stage(0, 2)
    send_router(2)
    send_sums(3, 3)
    normalise(3)
    stage(3, 0)
    stage(2, 1)
    stage(1, 2)

    stage(3, 1)
    stage(2, 2)
    stage(3, 2)

    def order_of(index):
        source = lax.broadcasted_iota(jnp.int32, (128, 256), 0)
        target = lax.broadcasted_iota(jnp.int32, (128, 256), 1)
        place = lax.rem(source, 32) * 8 + index * 4 + source // 32
        return jnp.where((place == target) & (lax.rem(source, 32) < TILES), 1.0, 0.0)

    in_rows = sum(
        jnp.dot(
            scales[:, index],
            order_of(index),
            precision=lax.Precision.HIGHEST,
            preferred_element_type=jnp.float32,
        )
        for index in range(2)
    )
    scale[...] = in_rows[:, 0 : TILES * 8]

    for e in range(EXPERTS):
        for s in range(3):
            wait_bytes(arrivals(e, s), sums_send.at[e, s])
    for e in range(EXPERTS):
        for p in range(3):
            for copy in first_copies(e, p) + second_copies(e, p):
                copy.wait_send()
            wait_bytes(third_bytes(e, p), part_send.at[e, p, 2, 0])
            wait_bytes(third_bytes(e, p), part_recv.at[e, p, 2, 0])
    for k in range(1, 4):
        ep_copy(k).wait_send()
    for s in range(3):
        for copy in router_copies(s):
            copy.wait_send()
            if s == 2:
                copy.wait_recv()


def exchange(master, second, weight, gain):
    vmem = pl.BlockSpec(memory_space=pltpu.VMEM)
    hbm = pl.BlockSpec(memory_space=pltpu.HBM)
    rows = EXPERTS, GROUP * TILES, 8, 128
    part_bufs = []
    for order, _, count in PARTS:
        a, b, c = (SIZES[dim] for dim in order)
        part_bufs.append(
            pltpu.VMEM((EXPERTS, 2 * a - 1, 2 * b - 1, c, count, 8, 128), jnp.bfloat16)
        )
    dma = pltpu.SemaphoreType.DMA
    return pl.pallas_call(
        kernel,
        name="exchange",
        out_shape=(
            pltpu.VMEM((EXPERTS, TILES, 8, GROUP * 128), jnp.bfloat16),
            pltpu.VMEM((EXPERTS, TILES * 8), jnp.float32),
            pltpu.VMEM((16, GROUP * 128), jnp.bfloat16),
        ),
        in_specs=[hbm, hbm, vmem, vmem],
        out_specs=(vmem, vmem, vmem),
        scratch_shapes=[
            pltpu.VMEM(rows, jnp.float32),
            pltpu.VMEM(rows, jnp.bfloat16),
            *part_bufs,
            pltpu.VMEM((EXPERTS, 4, GROUP // 4, 8, 128), jnp.float32),
            pltpu.VMEM((EXPERTS, 7, GROUP // 4, 8, 128), jnp.float32),
            pltpu.VMEM((EXPERTS, GROUP // 4, 8, 128), jnp.float32),
            pltpu.VMEM((EXPERTS, 2, 128), jnp.float32),
            pltpu.VMEM((4, 4, 128), jnp.float32),
            dma((2, EXPERTS)),
            dma((EXPERTS, 3)),
            dma((EXPERTS, 3)),
            dma((EXPERTS, 3, 3, 3)),
            dma((EXPERTS, 3, 3, 3)),
            dma((4,)),
            dma((4,)),
            dma((3, 3)),
            dma((3, 3)),
        ],
        compiler_params=pltpu.CompilerParams(
            collective_id=0, has_side_effects=True, vmem_limit_bytes=48 * 2**20
        ),
    )(
        master.reshape(rows),
        second.reshape(rows),
        weight.T,
        gain.reshape(1, 128),
    )


def write_out(final, scale, serve, final_out, scale_out, serve_out, sem):
    copies = [
        pltpu.make_async_copy(serve, serve_out, sem.at[2 * EXPERTS]),
        pltpu.make_async_copy(scale, scale_out, sem.at[2 * EXPERTS + 1]),
    ]
    for e in range(EXPERTS):
        for h, tiles in enumerate((pl.ds(0, 13), pl.ds(13, 12))):
            copies.append(
                pltpu.make_async_copy(
                    final.at[e, tiles], final_out.at[e, tiles], sem.at[2 * e + h]
                )
            )
    for copy in copies:
        copy.start()
    for copy in copies:
        copy.wait()


def written(final, scale, serve):
    vmem = pl.BlockSpec(memory_space=pltpu.VMEM)
    hbm = pl.BlockSpec(memory_space=pltpu.HBM)
    return pl.pallas_call(
        write_out,
        name="write_out",
        out_shape=tuple(
            jax.ShapeDtypeStruct(value.shape, value.dtype) for value in (final, scale, serve)
        ),
        in_specs=[vmem] * 3,
        out_specs=(hbm,) * 3,
        scratch_shapes=[pltpu.SemaphoreType.DMA((2 * EXPERTS + 2,))],
        compiler_params=pltpu.CompilerParams(vmem_limit_bytes=16 * 2**20),
    )(final, scale, serve)


def shards(master_down, second_down, router_weight, router_gain):
    final, scale, serve = written(
        *exchange(master_down, second_down, router_weight, router_gain)
    )
    return final.reshape(EXPERTS, TILES * 8, GROUP * 128), scale, serve.T


def solution(mesh):
    return jax.shard_map(
        shards,
        mesh=mesh,
        in_specs=(P("ep", None, "fsdp"), P("ep", None, "fsdp"), P("fsdp", "ep"), P("fsdp")),
        out_specs=(P("ep", "fsdp", None), P("ep", "fsdp"), P()),
        check_vma=False,
    )
```
